512 devices in a mesh: gx: 32 (over x_lo, y, core), gy: 16 (over z, x_hi).
Axes of the slice: x: 4 (x_hi: 2, x_lo: 2; x = x_hi * 2 + x_lo), y: 8, z: 8, core: 2. Of those that a mesh axis runs over, the one named last changes fastest.
Arguments:
- probe_signs: int32 [32, 64, 256, 128], P(None, 'gx', 'gy'), may hold values from 0 to 1
- diagonal: float32 [64, 256, 128], P('gx', 'gy'), may hold values from 0.25 to 4
Outputs:
- diagonal_blocks: float32 [3, 32, 32], replicated
- offdiag_blocks: float32 [3, 32, 32], replicated
- next_block: float32 [32, 64, 256, 128], P(None, 'gx', 'gy')
The draws below stay inside these ranges and needn't reach their ends.
All inputs are finite; a program needn't handle non-finite values.
Results may differ from the reference program's by a relative error of at most 0.0006.
Values sent between devices are 32-bit elements; how exact they have to be, the bound alone decides.
No kernel may reach another device: no remote copies, remote signals or barrier semaphores. Data moves between devices by JAX's collectives and lax.ppermute only.
A program may use at most 64 MiB of HBM per device.

```python
import math
import jax
import jax.numpy as jnp
from jax import lax

PROBES = 32
ITERS = 3
NX = 64
NY = 256
NZ = 128


def draw_probe_signs(key, part):
    common_bits = jax.random.randint(jax.random.fold_in(key, 11), (1, NX, NY, NZ), 0, 2)
    flip_limits = jax.random.randint(jax.random.fold_in(key, 12), (PROBES, 1, 1, 1), 15, 36)
    percent_draws = jax.random.randint(jax.random.fold_in(key, 13), (PROBES, NX, NY, NZ), 0, 100)
    flipped = (percent_draws < flip_limits).astype(jnp.int32)
    return ((common_bits + flipped) % 2).astype(jnp.int32)


def block_scale(own_key, extent, split, low, top_value):
    level, own = 1.0, jax.random.fold_in(own_key, 6)
    for dim, blocks in split:
        steps = jnp.exp(jax.random.uniform(jax.random.fold_in(own, dim), (blocks,), jnp.float32, low / len(split), top_value / len(split)))
        level = level * jnp.repeat(steps, extent[dim] // blocks).reshape([-1 if axis == dim else 1 for axis in range(len(extent))])
    return level


def setup_inputs(seed: int = 0) -> dict:
    keys = jax.random.split(jax.random.key(seed), 3)
    return {
        "probe_signs": draw_probe_signs(jax.random.fold_in(keys[2], 71), 0),
        "diagonal": jnp.clip(jnp.exp(math.log(4.0) - 2.7725887 * jax.random.uniform(keys[1], (NX, NY, NZ), jnp.float32) ** block_scale(keys[1], (NX, NY, NZ), ((0, 32), (1, 16)), -0.2, 0.2)), 0.25, 4.0),
    }


def stencil(vectors, diagonal):
    beside = jnp.roll(vectors, 1, 1) + jnp.roll(vectors, -1, 1)
    beside = beside + jnp.roll(vectors, 1, 2) + jnp.roll(vectors, -1, 2)
    beside = beside + jnp.roll(vectors, 1, 3) + jnp.roll(vectors, -1, 3)
    return (6.0 + diagonal)[None] * vectors - beside

def inner_block(left, right):
    return jnp.einsum('pxyz,qxyz->pq', left, right, precision=lax.Precision.HIGHEST)

def combine(vectors, matrix):
    return jnp.einsum('pxyz,pq->qxyz', vectors, matrix, precision=lax.Precision.HIGHEST)

def inverse_lower(gram_matrix):
    lower_factor = jnp.linalg.cholesky(gram_matrix)
    identity_matrix = jnp.eye(gram_matrix.shape[0], dtype=gram_matrix.dtype)
    inverse = lax.linalg.triangular_solve(lower_factor, identity_matrix, left_side=True, lower=True)
    return (lower_factor, inverse)

def reference(probe_signs, diagonal):
    scale_factor = 1.0 / jnp.sqrt(jnp.float32(NX * NY * NZ))
    probes = (2.0 * probe_signs.astype(jnp.float32) - 1.0) * scale_factor
    lower_factor, inverse = inverse_lower(inner_block(probes, probes))
    current = combine(probes, inverse.T)
    previous = None
    coupling = None
    alphas = []
    betas = []
    for iteration in range(ITERS):
        image = stencil(current, diagonal)
        if previous is not None:
            image = image - combine(previous, coupling)
        projected = inner_block(current, image)
        remain = image - combine(current, projected)
        lower_factor, inverse = inverse_lower(inner_block(remain, remain))
        alphas.append(projected)
        betas.append(lower_factor.T)
        previous = current
        coupling = lower_factor
        current = combine(remain, inverse.T)
    return (jnp.stack(alphas), jnp.stack(betas), current)
```

```python
import functools

import jax
import jax.numpy as jnp
from jax import lax
from jax.experimental import pallas as pl
from jax.experimental.pallas import tpu as pltpu
from jax.sharding import Mesh
from jax.sharding import PartitionSpec as P

GX = ("gx_0", "gx_1", "gx_2")
GY = ("gy_0", "gy_1")
NEAR = ("gx_0", "gx_2", "gy_1")
FAR = ("gx_1", "gy_0")

PROBES = 32
LANES = 128
ROWS = 16
PLANES = 2
CELLS = PLANES * ROWS
SHIFT = 7.75
B0 = 7.0
B1 = 10.0
PANEL = 8
F32 = jnp.float32
BF16 = jnp.bfloat16
INTERPRET = False

Y_ROWS = 2 * 3 * PROBES
X_BLOCKS = 20 + 18
X_ROWS = X_BLOCKS * PROBES


def vmem_specs(count):
    return [pl.BlockSpec(memory_space=pltpu.VMEM) for _ in range(count)]


def shaped(*shape, dtype=F32):
    return jax.ShapeDtypeStruct(shape, dtype)


def row_of(index):
    return pl.ds(index * PROBES, PROBES)


def prepare_kernel(signs_ref, diag_ref, own_ref, up_ref, down_ref):
    for cell in range(CELLS):
        plane, row = divmod(cell, ROWS)
        bits = signs_ref[pl.ds(cell, PROBES, stride=CELLS), :]
        probes = (2 * bits - 1).astype(F32)
        own_ref[row_of(cell), :] = probes
        if row < 3:
            down_ref[row_of(plane * 3 + row), :] = probes
        if row >= ROWS - 3:
            up_ref[row_of(plane * 3 + row - (ROWS - 3)), :] = probes
    for plane in range(PLANES):
        base = plane * ROWS
        down_ref[Y_ROWS + 2 * plane : Y_ROWS + 2 * plane + 2, :] = diag_ref[base : base + 2, :]
        up_ref[Y_ROWS + 2 * plane : Y_ROWS + 2 * plane + 2, :] = diag_ref[base + ROWS - 2 : base + ROWS, :]
    down_ref[Y_ROWS + 4 : Y_ROWS + 8, :] = jnp.zeros((4, LANES), F32)
    up_ref[Y_ROWS + 4 : Y_ROWS + 8, :] = jnp.zeros((4, LANES), F32)


def prepare(signs, diagonal):
    return pl.pallas_call(
        prepare_kernel,
        out_shape=(shaped(CELLS * PROBES, LANES), shaped(Y_ROWS + 8, LANES), shaped(Y_ROWS + 8, LANES)),
        in_specs=vmem_specs(2),
        out_specs=tuple(vmem_specs(3)),
        interpret=INTERPRET,
        name="prepare",
    )(signs, diagonal)


def pack_kernel(own_ref, diag_ref, low_ref, high_ref, plus_ref, minus_ref):
    def cell_of(plane, row):
        if row < 0:
            return low_ref[row_of(plane * 3 + row + 3), :]
        if row >= ROWS:
            return high_ref[row_of(plane * 3 + row - ROWS), :]
        return own_ref[row_of(plane * ROWS + row), :]

    def diag_of(plane, row):
        if row < 0:
            start = Y_ROWS + 2 * plane + row + 2
            return low_ref[start : start + 1, :]
        if row >= ROWS:
            start = Y_ROWS + 2 * plane + row - ROWS
            return high_ref[start : start + 1, :]
        return diag_ref[plane * ROWS + row : plane * ROWS + row + 1, :]

    for ref, near in ((plus_ref, 1), (minus_ref, 0)):
        far = 1 - near
        block = 0
        for row in range(-2, ROWS + 2):
            ref[row_of(block), :] = cell_of(near, row)
            block += 1
        for row in range(-1, ROWS + 1):
            ref[row_of(block), :] = cell_of(far, row)
            block += 1
        line = X_ROWS
        for row in range(-1, ROWS + 1):
            ref[line : line + 1, :] = diag_of(near, row)
            line += 1
        for row in range(ROWS):
            ref[line : line + 1, :] = diag_of(far, row)
            line += 1
        ref[line : line + 6, :] = jnp.zeros((6, LANES), F32)


def pack(own, diagonal, low, high):
    return pl.pallas_call(
        pack_kernel,
        out_shape=(shaped(X_ROWS + 40, LANES), shaped(X_ROWS + 40, LANES)),
        in_specs=vmem_specs(4),
        out_specs=tuple(vmem_specs(2)),
        interpret=INTERPRET,
        name="pack",
    )(own, diagonal, low, high)


def nt_dot(left, right, precision=None):
    return lax.dot_general(
        left, right, (((1,), (1,)), ((), ())), precision=precision, preferred_element_type=F32
    )


def basis_kernel(
    own_ref, diag_ref, low_ref, high_ref, left_ref, right_ref, left2_ref, right2_ref,
    high_out, low_out, gram_ref, first_ref, second_ref,
):
    def distance(plane):
        return -plane if plane < 0 else max(plane - (PLANES - 1), 0)

    def k0(plane, row):
        away = distance(plane)
        if away == 0:
            if row < 0:
                return low_ref[row_of(plane * 3 + row + 3), :]
            if row >= ROWS:
                return high_ref[row_of(plane * 3 + row - ROWS), :]
            return own_ref[row_of(plane * ROWS + row), :]
        side, side2 = (left_ref, left2_ref) if plane < 0 else (right_ref, right2_ref)
        if away == 1:
            return side[row_of(row + 2), :]
        if away == 2:
            return side[row_of(20 + row + 1), :]
        return side2[row_of(row), :]

    def factor(plane, row):
        away = distance(plane)
        if away == 0:
            if row < 0:
                start = Y_ROWS + 2 * plane + row + 2
                line = low_ref[start : start + 1, :]
            elif row >= ROWS:
                start = Y_ROWS + 2 * plane + row - ROWS
                line = high_ref[start : start + 1, :]
            else:
                line = diag_ref[plane * ROWS + row : plane * ROWS + row + 1, :]
        else:
            side = left_ref if plane < 0 else right_ref
            start = X_ROWS + (row + 1 if away == 1 else 18 + row)
            line = side[start : start + 1, :]
        return line + (6.0 - SHIFT)

    def cells(width):
        found = []
        for plane in range(-width, PLANES + width):
            extra = width - distance(plane)
            for row in range(-extra, ROWS + extra):
                found.append((plane, row))
        return found

    first_slot = {key: slot for slot, key in enumerate(cells(2))}
    second_slot = {key: slot for slot, key in enumerate(cells(1))}

    def k1(plane, row):
        return first_ref[row_of(first_slot[(plane, row)]), :]

    def k2(plane, row):
        return second_ref[row_of(second_slot[(plane, row)]), :]

    def apply(field, plane, row):
        center = field(plane, row)
        beside = field(plane - 1, row) + field(plane + 1, row)
        beside = beside + (field(plane, row - 1) + field(plane, row + 1))
        beside = beside + (pltpu.roll(center, 1, 1) + pltpu.roll(center, LANES - 1, 1))
        return factor(plane, row) * center - beside

    def keep(order, plane, row, value):
        columns = pl.ds((plane * ROWS + row) * LANES, LANES)
        upper = value.astype(BF16)
        high_out[row_of(order), columns] = upper
        if order == 0:
            low_out[row_of(order), columns] = jnp.zeros_like(upper)
        else:
            low_out[row_of(order), columns] = (value - upper.astype(F32)).astype(BF16)

    for plane, row in cells(0):
        keep(0, plane, row, k0(plane, row))
    for plane, row in cells(2):
        value = apply(k0, plane, row)
        first_ref[row_of(first_slot[(plane, row)]), :] = value
        if distance(plane) == 0 and 0 <= row < ROWS:
            keep(1, plane, row, value)
    for plane, row in cells(1):
        value = apply(k1, plane, row) - B0 * k0(plane, row)
        second_ref[row_of(second_slot[(plane, row)]), :] = value
        if distance(plane) == 0 and 0 <= row < ROWS:
            keep(2, plane, row, value)
    for plane, row in cells(0):
        keep(3, plane, row, apply(k2, plane, row) - B1 * k1(plane, row))
    upper = high_out[...]
    lower = low_out[...]
    top = nt_dot(upper[:PROBES], upper) + nt_dot(upper[:PROBES], lower)
    bottom = nt_dot(upper[3 * PROBES :], upper) + nt_dot(upper[3 * PROBES :], lower)
    gram_ref[:PROBES, :] = top
    gram_ref[PROBES:, :] = bottom + nt_dot(lower[3 * PROBES :], upper)


def basis(*operands):
    width = CELLS * LANES
    return pl.pallas_call(
        basis_kernel,
        out_shape=(
            shaped(4 * PROBES, width, dtype=BF16),
            shaped(4 * PROBES, width, dtype=BF16),
            shaped(2 * PROBES, LANES),
        ),
        in_specs=vmem_specs(len(operands)),
        out_specs=tuple(vmem_specs(3)),
        scratch_shapes=[pltpu.VMEM((108 * PROBES, LANES), F32), pltpu.VMEM((68 * PROBES, LANES), F32)],
        interpret=INTERPRET,
        name="basis",
    )(*operands)


def eliminate(system, block):
    groups = PROBES // 8
    lane = lax.broadcasted_iota(jnp.int32, (8, LANES), 1)
    sub = lax.broadcasted_iota(jnp.int32, (8, LANES), 0)
    start = block * PROBES
    inside = (lane >= start) & (lane < start + PROBES)
    pivoted = [system[8 * g : 8 * g + 8, :] for g in range(groups)]
    solved = [
        jnp.where(inside, jnp.where(lane - start == sub + 8 * g, 1.0, 0.0), pivoted[g]) for g in range(groups)
    ]
    scales = [None] * PROBES
    for panel in range(0, PROBES, PANEL):
        first_group = panel // 8
        spread = {}
        for k in range(panel, panel + PANEL):
            for g in range(first_group, groups):
                column = pivoted[g][:, start + k : start + k + 1]
                spread[k, g] = jnp.broadcast_to(column, (8, LANES))
        for k in range(panel, panel + PANEL):
            group, line = divmod(k, 8)

            def pivot_row(value):
                return jnp.broadcast_to(value[line : line + 1, :], (8, LANES))

            pivot = pivot_row(spread[k, group])
            inverse = 1.0 / pivot
            scales[k] = lax.rsqrt(pivot)
            multiplier = {}
            for g in range(group, groups):
                value = spread[k, g] * inverse
                if g == group:
                    value = jnp.where(sub > line, value, 0.0)
                multiplier[g] = value
            for other in range(k + 1, panel + PANEL):
                row = pivot_row(spread[other, group])
                for g in range(group, groups):
                    spread[other, g] = spread[other, g] - multiplier[g] * row
            row = pivot_row(pivoted[group])
            solved_row = pivot_row(solved[group])
            for g in range(group, groups):
                pivoted[g] = pivoted[g] - multiplier[g] * row
                solved[g] = solved[g] - multiplier[g] * solved_row
    upper = []
    for g in range(groups):
        scale = scales[8 * g]
        for line in range(1, 8):
            scale = jnp.where(sub == line, scales[8 * g + line], scale)
        solved[g] = solved[g] * scale
        upper.append(jnp.where(inside & (lane - start >= sub + 8 * g), pivoted[g] * scale, 0.0))
    return jnp.concatenate(solved, 0), jnp.concatenate(upper, 0)


def finish_kernel(gram_ref, high_ref, low_ref, alpha_ref, beta_ref, next_ref):
    exact = lax.Precision.HIGHEST
    lane = lax.broadcasted_iota(jnp.int32, (PROBES, LANES), 1)
    block_of = lane // PROBES
    first = gram_ref[:PROBES, :]
    last = gram_ref[PROBES:, :]

    def moved(value, blocks):
        return pltpu.roll(value, (blocks * PROBES) % LANES, 1)

    second = moved(first, -1) + jnp.where(block_of == 1, B0, B1) * moved(first, 1)
    second = jnp.where(block_of == 3, moved(last, 2), jnp.where(block_of == 0, 0.0, second))
    third = moved(last, 1) + jnp.where(block_of == 2, B1 * moved(second, 1) - B0 * first, 0.0)
    third = jnp.where(block_of < 2, 0.0, third)
    systems = [first, second, third, jnp.where(block_of < 3, 0.0, last)]
    solved = []
    uppers = []
    for block in range(4):
        value, upper = eliminate(systems[block], block)
        solved.append(value)
        uppers.append(upper)
        if block < 3:
            tail = value[:, (block + 1) * PROBES :]
            update = lax.dot_general(
                tail, value, (((0,), (0,)), ((), ())), precision=exact, preferred_element_type=F32
            )
            for later in range(block + 1, 4):
                offset = (later - block - 1) * PROBES
                change = update[offset : offset + PROBES, :]
                change = jnp.where((block_of <= block) | (block_of >= later), change, 0.0)
                systems[later] = systems[later] - change
    weights = solved[3]
    upper = weights.astype(BF16)
    lower = (weights - upper.astype(F32)).astype(BF16)
    high = high_ref[...]
    result = jnp.dot(upper, high, preferred_element_type=F32)
    result = result + jnp.dot(upper, low_ref[...], preferred_element_type=F32)
    result = result + jnp.dot(lower, high, preferred_element_type=F32)
    for cell in range(CELLS):
        next_ref[pl.ds(cell, PROBES, stride=CELLS), :] = result[:, cell * LANES : (cell + 1) * LANES]
    row32 = lax.broadcasted_iota(jnp.int32, (PROBES, PROBES), 0)
    lane32 = lax.broadcasted_iota(jnp.int32, (PROBES, PROBES), 1)
    beta = None
    for block in range(3):
        inverse = jnp.where(block_of == block, solved[block], 0.0)
        alpha = nt_dot(moved(solved[block], -1), inverse, exact)
        if block > 0:
            alpha = alpha - jnp.dot(
                beta, nt_dot(solved[block - 1], inverse, exact), precision=exact, preferred_element_type=F32
            )
        alpha_ref[block] = alpha + jnp.where(row32 == lane32, SHIFT, 0.0)
        beta = nt_dot(moved(uppers[block + 1], -1), inverse, exact)
        beta_ref[block] = jnp.where(row32 <= lane32, beta, 0.0)


def finish(gram, high, low):
    return pl.pallas_call(
        finish_kernel,
        out_shape=(
            shaped(3, PROBES, PROBES),
            shaped(3, PROBES, PROBES),
            shaped(PROBES * CELLS, LANES),
        ),
        in_specs=vmem_specs(3),
        out_specs=tuple(vmem_specs(3)),
        interpret=INTERPRET,
        name="finish",
    )(gram, high, low)


def shifted(x, axes, steps):
    count = lax.axis_size(axes)
    return lax.ppermute(x, axes, [(i, (i + steps) % count) for i in range(count)])


def exchanged(x, axes):
    return lax.all_to_all(x, axes, 0, 0, tiled=True)


def gathered(x, axes):
    return exchanged(jnp.broadcast_to(x[None], (lax.axis_size(axes),) + x.shape), axes)


def reduced(x):
    near = lax.axis_size(NEAR)
    part = exchanged(x.reshape(near, x.shape[0] // near, x.shape[1]), NEAR).sum(0)
    part = gathered(part, FAR).sum(0)
    return gathered(part, NEAR).reshape(x.shape)


def per_device(probe_signs, diagonal):
    signs = probe_signs.reshape(PROBES * CELLS, LANES)
    diag = diagonal.reshape(CELLS, LANES)
    own, up, down = prepare(signs, diag)
    low = shifted(up, GY, 1)
    high = shifted(down, GY, -1)
    half = ROWS * PROBES
    left2 = shifted(own[half:], GX, 2)
    right2 = shifted(own[:half], GX, -2)
    plus, minus = pack(own, diag, low, high)
    left = shifted(plus, GX, 1)
    right = shifted(minus, GX, -1)
    upper, lower, gram = basis(own, diag, low, high, left, right, left2, right2)
    alphas, betas, following = finish(reduced(gram), upper, lower)
    return (alphas, betas, following.reshape(PROBES, PLANES, ROWS, LANES))


def solution(mesh):
    split = Mesh(mesh.devices.reshape(2, 8, 2, 8, 2), ("gx_0", "gx_1", "gx_2", "gy_0", "gy_1"))
    placed = (P(None, GX, GY, None), P(GX, GY, None))
    return jax.shard_map(
        per_device,
        mesh=split,
        in_specs=placed,
        out_specs=(P(), P(), P(None, GX, GY, None)),
        check_vma=False,
    )
```

```python
import jax
import jax.numpy as jnp
from jax import lax
from jax.experimental import pallas as pl
from jax.experimental.pallas import tpu as pltpu
from jax.sharding import Mesh
from jax.sharding import PartitionSpec as P


GX = ("gx_0", "gx_1", "gx_2")
GY = ("gy_0", "gy_1")
NEAR = ("gx_0", "gx_2", "gy_1")
FAR = ("gx_1", "gy_0")

PROBES = 32
LANES = 128
ROWS = 16
PLANES = 2
CELLS = PLANES * ROWS
SHIFT = 7.75
B0 = 7.0
B1 = 10.0
PANEL = 8
F32 = jnp.float32
BF16 = jnp.bfloat16
INTERPRET = False
VMEM_LIMIT = 16 * 2**20

Y_ROWS = 2 * 3 * PROBES
X_BLOCKS = 20 + 18
X_ROWS = X_BLOCKS * PROBES


def vmem_specs(count):
    return [pl.BlockSpec(memory_space=pltpu.VMEM) for _ in range(count)]


def shaped(*shape, dtype=F32):
    return pltpu.VMEM(shape, dtype)


def held(*arrays):
    return tuple(pltpu.with_memory_space_constraint(x, pltpu.VMEM) for x in arrays)


def row_of(index):
    return pl.ds(index * PROBES, PROBES)


def prepare_kernel(signs_ref, diag_ref, own_ref, up_ref, down_ref):
    for cell in range(CELLS):
        plane, row = divmod(cell, ROWS)
        bits = signs_ref[pl.ds(cell, PROBES, stride=CELLS), :]
        probes = (2 * bits - 1).astype(F32)
        own_ref[row_of(cell), :] = probes
        if row < 3:
            down_ref[row_of(plane * 3 + row), :] = probes
        if row >= ROWS - 3:
            up_ref[row_of(plane * 3 + row - (ROWS - 3)), :] = probes
    for plane in range(PLANES):
        base = plane * ROWS
        down_ref[Y_ROWS + 2 * plane : Y_ROWS + 2 * plane + 2, :] = diag_ref[base : base + 2, :]
        up_ref[Y_ROWS + 2 * plane : Y_ROWS + 2 * plane + 2, :] = diag_ref[base + ROWS - 2 : base + ROWS, :]
    down_ref[Y_ROWS + 4 : Y_ROWS + 8, :] = jnp.zeros((4, LANES), F32)
    up_ref[Y_ROWS + 4 : Y_ROWS + 8, :] = jnp.zeros((4, LANES), F32)


def prepare(signs, diagonal):
    return pl.pallas_call(
        prepare_kernel,
        out_shape=(shaped(CELLS * PROBES, LANES), shaped(Y_ROWS + 8, LANES), shaped(Y_ROWS + 8, LANES)),
        in_specs=vmem_specs(2),
        out_specs=tuple(vmem_specs(3)),
        compiler_params=pltpu.CompilerParams(vmem_limit_bytes=VMEM_LIMIT),
        interpret=INTERPRET,
        name="prepare",
    )(signs, diagonal)


def pack_kernel(own_ref, diag_ref, low_ref, high_ref, plus_ref, minus_ref):
    def cell_of(plane, row):
        if row < 0:
            return low_ref[row_of(plane * 3 + row + 3), :]
        if row >= ROWS:
            return high_ref[row_of(plane * 3 + row - ROWS), :]
        return own_ref[row_of(plane * ROWS + row), :]

    def diag_of(plane, row):
        if row < 0:
            start = Y_ROWS + 2 * plane + row + 2
            return low_ref[start : start + 1, :]
        if row >= ROWS:
            start = Y_ROWS + 2 * plane + row - ROWS
            return high_ref[start : start + 1, :]
        return diag_ref[plane * ROWS + row : plane * ROWS + row + 1, :]

    for ref, near in ((plus_ref, 1), (minus_ref, 0)):
        far = 1 - near
        block = 0
        for row in range(-2, ROWS + 2):
            ref[row_of(block), :] = cell_of(near, row)
            block += 1
        for row in range(-1, ROWS + 1):
            ref[row_of(block), :] = cell_of(far, row)
            block += 1
        line = X_ROWS
        for row in range(-1, ROWS + 1):
            ref[line : line + 1, :] = diag_of(near, row)
            line += 1
        for row in range(ROWS):
            ref[line : line + 1, :] = diag_of(far, row)
            line += 1
        ref[line : line + 6, :] = jnp.zeros((6, LANES), F32)


def pack(own, diagonal, low, high):
    return pl.pallas_call(
        pack_kernel,
        out_shape=(shaped(X_ROWS + 40, LANES), shaped(X_ROWS + 40, LANES)),
        in_specs=vmem_specs(4),
        out_specs=tuple(vmem_specs(2)),
        compiler_params=pltpu.CompilerParams(vmem_limit_bytes=VMEM_LIMIT),
        interpret=INTERPRET,
        name="pack",
    )(*held(own), diagonal, *held(low, high))


def nt_dot(left, right, precision=None):
    return lax.dot_general(
        left, right, (((1,), (1,)), ((), ())), precision=precision, preferred_element_type=F32
    )


def basis_kernel(
    own_ref, diag_ref, low_ref, high_ref, left_ref, right_ref, left2_ref, right2_ref,
    high_out, low_out, gram_ref, first_ref, second_ref,
):
    def distance(plane):
        return -plane if plane < 0 else max(plane - (PLANES - 1), 0)

    def k0(plane, row):
        away = distance(plane)
        if away == 0:
            if row < 0:
                return low_ref[row_of(plane * 3 + row + 3), :]
            if row >= ROWS:
                return high_ref[row_of(plane * 3 + row - ROWS), :]
            return own_ref[row_of(plane * ROWS + row), :]
        side, side2 = (left_ref, left2_ref) if plane < 0 else (right_ref, right2_ref)
        if away == 1:
            return side[row_of(row + 2), :]
        if away == 2:
            return side[row_of(20 + row + 1), :]
        return side2[row_of(row), :]

    def factor(plane, row):
        away = distance(plane)
        if away == 0:
            if row < 0:
                start = Y_ROWS + 2 * plane + row + 2
                line = low_ref[start : start + 1, :]
            elif row >= ROWS:
                start = Y_ROWS + 2 * plane + row - ROWS
                line = high_ref[start : start + 1, :]
            else:
                line = diag_ref[plane * ROWS + row : plane * ROWS + row + 1, :]
        else:
            side = left_ref if plane < 0 else right_ref
            start = X_ROWS + (row + 1 if away == 1 else 18 + row)
            line = side[start : start + 1, :]
        return line + (6.0 - SHIFT)

    def cells(width):
        found = []
        for plane in range(-width, PLANES + width):
            extra = width - distance(plane)
            for row in range(-extra, ROWS + extra):
                found.append((plane, row))
        return found

    first_slot = {key: slot for slot, key in enumerate(cells(2))}
    second_slot = {key: slot for slot, key in enumerate(cells(1))}

    def k1(plane, row):
        return first_ref[row_of(first_slot[(plane, row)]), :]

    def k2(plane, row):
        return second_ref[row_of(second_slot[(plane, row)]), :]

    def apply(field, plane, row):
        center = field(plane, row)
        beside = field(plane - 1, row) + field(plane + 1, row)
        beside = beside + (field(plane, row - 1) + field(plane, row + 1))
        beside = beside + (pltpu.roll(center, 1, 1) + pltpu.roll(center, LANES - 1, 1))
        return factor(plane, row) * center - beside

    def keep(order, plane, row, value):
        columns = pl.ds((plane * ROWS + row) * LANES, LANES)
        upper = value.astype(BF16)
        high_out[row_of(order), columns] = upper
        if order == 0:
            low_out[row_of(order), columns] = jnp.zeros_like(upper)
        else:
            low_out[row_of(order), columns] = (value - upper.astype(F32)).astype(BF16)

    for plane, row in cells(0):
        keep(0, plane, row, k0(plane, row))
    for plane, row in cells(2):
        value = apply(k0, plane, row)
        first_ref[row_of(first_slot[(plane, row)]), :] = value
        if distance(plane) == 0 and 0 <= row < ROWS:
            keep(1, plane, row, value)
    for plane, row in cells(1):
        value = apply(k1, plane, row) - B0 * k0(plane, row)
        second_ref[row_of(second_slot[(plane, row)]), :] = value
        if distance(plane) == 0 and 0 <= row < ROWS:
            keep(2, plane, row, value)
    for plane, row in cells(0):
        keep(3, plane, row, apply(k2, plane, row) - B1 * k1(plane, row))
    upper = high_out[...]
    lower = low_out[...]
    top = nt_dot(upper[:PROBES], upper) + nt_dot(upper[:PROBES], lower)
    bottom = nt_dot(upper[3 * PROBES :], upper) + nt_dot(upper[3 * PROBES :], lower)
    gram_ref[:PROBES, :] = top
    gram_ref[PROBES:, :] = bottom + nt_dot(lower[3 * PROBES :], upper)


def basis(*operands):
    width = CELLS * LANES
    return pl.pallas_call(
        basis_kernel,
        out_shape=(
            shaped(4 * PROBES, width, dtype=BF16),
            shaped(4 * PROBES, width, dtype=BF16),
            shaped(2 * PROBES, LANES),
        ),
        in_specs=vmem_specs(len(operands)),
        out_specs=tuple(vmem_specs(3)),
        scratch_shapes=[pltpu.VMEM((108 * PROBES, LANES), F32), pltpu.VMEM((68 * PROBES, LANES), F32)],
        compiler_params=pltpu.CompilerParams(vmem_limit_bytes=VMEM_LIMIT),
        interpret=INTERPRET,
        name="basis",
    )(*held(*operands))


def eliminate(system, block):
    groups = PROBES // 8
    lane = lax.broadcasted_iota(jnp.int32, (8, LANES), 1)
    sub = lax.broadcasted_iota(jnp.int32, (8, LANES), 0)
    start = block * PROBES
    inside = (lane >= start) & (lane < start + PROBES)
    pivoted = [system[8 * g : 8 * g + 8, :] for g in range(groups)]
    solved = [
        jnp.where(inside, jnp.where(lane - start == sub + 8 * g, 1.0, 0.0), pivoted[g]) for g in range(groups)
    ]
    scales = [None] * PROBES
    for panel in range(0, PROBES, PANEL):
        first_group = panel // 8
        spread = {}
        for k in range(panel, panel + PANEL):
            for g in range(first_group, groups):
                column = pivoted[g][:, start + k : start + k + 1]
                spread[k, g] = jnp.broadcast_to(column, (8, LANES))
        for k in range(panel, panel + PANEL):
            group, line = divmod(k, 8)

            def pivot_row(value):
                return jnp.broadcast_to(value[line : line + 1, :], (8, LANES))

            pivot = pivot_row(spread[k, group])
            inverse = 1.0 / pivot
            scales[k] = lax.rsqrt(pivot)
            multiplier = {}
            for g in range(group, groups):
                value = spread[k, g] * inverse
                if g == group:
                    value = jnp.where(sub > line, value, 0.0)
                multiplier[g] = value
            for other in range(k + 1, panel + PANEL):
                row = pivot_row(spread[other, group])
                for g in range(group, groups):
                    spread[other, g] = spread[other, g] - multiplier[g] * row
            row = pivot_row(pivoted[group])
            solved_row = pivot_row(solved[group])
            for g in range(group, groups):
                pivoted[g] = pivoted[g] - multiplier[g] * row
                solved[g] = solved[g] - multiplier[g] * solved_row
    upper = []
    for g in range(groups):
        scale = scales[8 * g]
        for line in range(1, 8):
            scale = jnp.where(sub == line, scales[8 * g + line], scale)
        solved[g] = solved[g] * scale
        upper.append(jnp.where(inside & (lane - start >= sub + 8 * g), pivoted[g] * scale, 0.0))
    return jnp.concatenate(solved, 0), jnp.concatenate(upper, 0)


def finish_kernel(gram_ref, high_ref, low_ref, alpha_ref, beta_ref, next_ref):
    exact = lax.Precision.HIGHEST
    lane = lax.broadcasted_iota(jnp.int32, (PROBES, LANES), 1)
    block_of = lane // PROBES
    first = gram_ref[:PROBES, :]
    last = gram_ref[PROBES:, :]

    def moved(value, blocks):
        return pltpu.roll(value, (blocks * PROBES) % LANES, 1)

    second = moved(first, -1) + jnp.where(block_of == 1, B0, B1) * moved(first, 1)
    second = jnp.where(block_of == 3, moved(last, 2), jnp.where(block_of == 0, 0.0, second))
    third = moved(last, 1) + jnp.where(block_of == 2, B1 * moved(second, 1) - B0 * first, 0.0)
    third = jnp.where(block_of < 2, 0.0, third)
    systems = [first, second, third, jnp.where(block_of < 3, 0.0, last)]
    solved = []
    uppers = []
    for block in range(4):
        value, upper = eliminate(systems[block], block)
        solved.append(value)
        uppers.append(upper)
        if block < 3:
            tail = value[:, (block + 1) * PROBES :]
            update = lax.dot_general(
                tail, value, (((0,), (0,)), ((), ())), precision=exact, preferred_element_type=F32
            )
            for later in range(block + 1, 4):
                offset = (later - block - 1) * PROBES
                change = update[offset : offset + PROBES, :]
                change = jnp.where((block_of <= block) | (block_of >= later), change, 0.0)
                systems[later] = systems[later] - change
    weights = solved[3]
    upper = weights.astype(BF16)
    lower = (weights - upper.astype(F32)).astype(BF16)
    high = high_ref[...]
    result = jnp.dot(upper, high, preferred_element_type=F32)
    result = result + jnp.dot(upper, low_ref[...], preferred_element_type=F32)
    result = result + jnp.dot(lower, high, preferred_element_type=F32)
    for cell in range(CELLS):
        next_ref[pl.ds(cell, PROBES, stride=CELLS), :] = result[:, cell * LANES : (cell + 1) * LANES]
    row32 = lax.broadcasted_iota(jnp.int32, (PROBES, PROBES), 0)
    lane32 = lax.broadcasted_iota(jnp.int32, (PROBES, PROBES), 1)
    beta = None
    for block in range(3):
        inverse = jnp.where(block_of == block, solved[block], 0.0)
        alpha = nt_dot(moved(solved[block], -1), inverse, exact)
        if block > 0:
            alpha = alpha - jnp.dot(
                beta, nt_dot(solved[block - 1], inverse, exact), precision=exact, preferred_element_type=F32
            )
        alpha_ref[block] = alpha + jnp.where(row32 == lane32, SHIFT, 0.0)
        beta = nt_dot(moved(uppers[block + 1], -1), inverse, exact)
        beta_ref[block] = jnp.where(row32 <= lane32, beta, 0.0)


def finish(gram, high, low):
    return pl.pallas_call(
        finish_kernel,
        out_shape=(
            jax.ShapeDtypeStruct((3, PROBES, PROBES), F32),
            jax.ShapeDtypeStruct((3, PROBES, PROBES), F32),
            jax.ShapeDtypeStruct((PROBES * CELLS, LANES), F32),
        ),
        in_specs=vmem_specs(3),
        out_specs=tuple(vmem_specs(3)),
        compiler_params=pltpu.CompilerParams(vmem_limit_bytes=VMEM_LIMIT),
        interpret=INTERPRET,
        name="finish",
    )(*held(gram, high, low))


def shifted(x, axes, steps):
    count = lax.axis_size(axes)
    return lax.ppermute(x, axes, [(i, (i + steps) % count) for i in range(count)])


def exchanged(x, axes):
    return lax.all_to_all(x, axes, 0, 0, tiled=True)


def gathered(x, axes):
    return exchanged(jnp.broadcast_to(x[None], (lax.axis_size(axes),) + x.shape), axes)


def reduced(x):
    near = lax.axis_size(NEAR)
    part = exchanged(x.reshape(near, x.shape[0] // near, x.shape[1]), NEAR).sum(0)
    part = gathered(part, FAR).sum(0)
    return gathered(part, NEAR).reshape(x.shape)


def per_device(probe_signs, diagonal):
    signs = probe_signs.reshape(PROBES * CELLS, LANES)
    diag = diagonal.reshape(CELLS, LANES)
    own, up, down = prepare(signs, diag)
    half = ROWS * PROBES
    low = shifted(up, GY, 1)
    high = shifted(down, GY, -1)
    left2 = shifted(own[half:], GX, 2)
    right2 = shifted(own[:half], GX, -2)
    plus, minus = pack(own, diag, low, high)
    left = shifted(plus, GX, 1)
    right = shifted(minus, GX, -1)
    upper, lower, gram = basis(own, diag, low, high, left, right, left2, right2)
    alphas, betas, following = finish(reduced(gram), upper, lower)
    return (alphas, betas, following.reshape(PROBES, PLANES, ROWS, LANES))


def solution(mesh):
    split = Mesh(mesh.devices.reshape(2, 8, 2, 8, 2), ("gx_0", "gx_1", "gx_2", "gy_0", "gy_1"))
    placed = (P(None, GX, GY, None), P(GX, GY, None))
    return jax.shard_map(
        per_device,
        mesh=split,
        in_specs=placed,
        out_specs=(P(), P(), P(None, GX, GY, None)),
        check_vma=False,
    )
```

```python
import jax
import jax.numpy as jnp
from jax import lax
from jax.experimental import pallas as pl
from jax.experimental.pallas import tpu as pltpu
from jax.sharding import Mesh
from jax.sharding import PartitionSpec as P


GX = ("gx_0", "gx_1", "gx_2")
GY = ("gy_0", "gy_1")
NEAR = ("gx_0", "gx_2", "gy_1")
FAR = ("gx_1", "gy_0")
CORE = "gx_2"

PROBES = 32
LANES = 128
ROWS = 16
PLANES = 2
CELLS = PLANES * ROWS
SHIFT = 7.75
B0 = 7.0
B1 = 10.0
PANEL = 8
F32 = jnp.float32
BF16 = jnp.bfloat16
INTERPRET = False
VMEM_LIMIT = 16 * 2**20

OWN_ROWS = CELLS * PROBES + CELLS
EDGE_ROWS = 2 * 3 * PROBES + 8
CORNER_ROWS = 6 * PROBES + 8
CROSS_ROWS = ROWS * PROBES + CORNER_ROWS


def vmem_specs(count):
    return [pl.BlockSpec(memory_space=pltpu.VMEM) for _ in range(count)]


def shaped(*shape, dtype=F32):
    return pltpu.VMEM(shape, dtype)


def held(*arrays):
    return tuple(pltpu.with_memory_space_constraint(x, pltpu.VMEM) for x in arrays)


def row_of(index):
    return pl.ds(index * PROBES, PROBES)


def prepare_kernel(mirror_ref, signs_ref, diag_ref, own_ref, far_ref, high_ref, low_ref):
    flip_plane = mirror_ref[0]
    flip_row = mirror_ref[1] * (ROWS - 1)
    for cell in range(CELLS):
        plane, row = divmod(cell, ROWS)
        source = (flip_plane ^ plane) * ROWS + (flip_row ^ row)
        bits = signs_ref[pl.ds(source, PROBES, stride=CELLS), :]
        probes = (2 * bits - 1).astype(F32)
        line = diag_ref[pl.ds(source, 1), :]
        own_ref[row_of(cell), :] = probes
        own_ref[CELLS * PROBES + cell : CELLS * PROBES + cell + 1, :] = line
        if plane == 1:
            far_ref[row_of(row), :] = probes
        for ref, step in ((low_ref, row), (high_ref, ROWS - 1 - row)):
            if step < 3:
                ref[row_of(plane * 3 + step), :] = probes
            if step < 2:
                start = 6 * PROBES + plane * 2 + step
                ref[start : start + 1, :] = line
    for ref in (low_ref, high_ref):
        ref[6 * PROBES + 4 :, :] = jnp.zeros((4, LANES), F32)


def prepare(mirror, signs, diagonal):
    return pl.pallas_call(
        prepare_kernel,
        out_shape=(
            shaped(OWN_ROWS, LANES),
            shaped(ROWS * PROBES, LANES),
            shaped(EDGE_ROWS, LANES),
            shaped(EDGE_ROWS, LANES),
        ),
        in_specs=[pl.BlockSpec(memory_space=pltpu.SMEM)] + vmem_specs(2),
        out_specs=tuple(vmem_specs(4)),
        compiler_params=pltpu.CompilerParams(vmem_limit_bytes=VMEM_LIMIT),
        interpret=INTERPRET,
        name="prepare",
    )(mirror, signs, diagonal)


def pack_kernel(high_ref, low_ref, near_ref, corner_ref, cross_ref):
    def edge(plane, row):
        if row < 0:
            return low_ref[row_of(plane * 3 - row - 1), :]
        return high_ref[row_of(plane * 3 + row - ROWS), :]

    def edge_line(plane, row):
        ref = low_ref if row < 0 else high_ref
        start = 6 * PROBES + plane * 2
        return ref[start : start + 1, :]

    for row in range(ROWS):
        cross_ref[row_of(row), :] = near_ref[row_of(row), :]
    for ref, plane, first in ((corner_ref, 0, 0), (cross_ref, 1, ROWS)):
        for place, row in enumerate((-2, -1, ROWS, ROWS + 1)):
            ref[row_of(first + place), :] = edge(plane, row)
        for place, row in enumerate((-1, ROWS)):
            ref[row_of(first + 4 + place), :] = edge(1 - plane, row)
            start = (first + 6) * PROBES + place
            ref[start : start + 1, :] = edge_line(plane, row)
        ref[(first + 6) * PROBES + 2 :, :] = jnp.zeros((6, LANES), F32)


def pack(high, low, near):
    return pl.pallas_call(
        pack_kernel,
        out_shape=(shaped(CORNER_ROWS, LANES), shaped(CROSS_ROWS, LANES)),
        in_specs=vmem_specs(3),
        out_specs=tuple(vmem_specs(2)),
        compiler_params=pltpu.CompilerParams(vmem_limit_bytes=VMEM_LIMIT),
        interpret=INTERPRET,
        name="pack",
    )(*held(high, low, near))


def nt_dot(left, right, precision=None):
    return lax.dot_general(
        left, right, (((1,), (1,)), ((), ())), precision=precision, preferred_element_type=F32
    )


def basis_kernel(
    own_ref, high_ref, low_ref, near_ref, beside_ref, far_ref, corner_ref, cross_ref,
    high_out, low_out, gram_ref, first_ref, second_ref,
):
    def distance(plane):
        return -plane if plane < 0 else max(plane - (PLANES - 1), 0)

    def k0(plane, row):
        away = distance(plane)
        if away == 0:
            if row < 0:
                return low_ref[row_of(plane * 3 - row - 1), :]
            if row >= ROWS:
                return high_ref[row_of(plane * 3 + row - ROWS), :]
            return own_ref[row_of(plane * ROWS + row), :]
        if away == 3:
            return (far_ref if plane < 0 else cross_ref)[row_of(row), :]
        if 0 <= row < ROWS:
            if plane < 0:
                return near_ref[row_of((away - 1) * ROWS + row), :]
            return beside_ref[row_of((2 - away) * ROWS + row), :]
        ref, first = (corner_ref, 0) if plane < 0 else (cross_ref, ROWS)
        places = (-2, -1, ROWS, ROWS + 1) if away == 1 else (-1, ROWS)
        return ref[row_of(first + 4 * (away - 1) + places.index(row)), :]

    def factor(plane, row):
        away = distance(plane)
        if away == 0:
            if row < 0:
                ref, start = low_ref, 6 * PROBES + plane * 2 - row - 1
            elif row >= ROWS:
                ref, start = high_ref, 6 * PROBES + plane * 2 + row - ROWS
            else:
                ref, start = own_ref, CELLS * PROBES + plane * ROWS + row
        elif 0 <= row < ROWS:
            if plane < 0:
                ref, start = near_ref, CELLS * PROBES + (away - 1) * ROWS + row
            else:
                ref, start = beside_ref, CELLS * PROBES + (2 - away) * ROWS + row
        else:
            ref, first = (corner_ref, 0) if plane < 0 else (cross_ref, ROWS)
            start = (first + 6) * PROBES + (0 if row < 0 else 1)
        return ref[start : start + 1, :] + (6.0 - SHIFT)

    def cells(width):
        found = []
        for plane in range(-width, PLANES + width):
            extra = width - distance(plane)
            for row in range(-extra, ROWS + extra):
                found.append((plane, row))
        return found

    first_slot = {key: slot for slot, key in enumerate(cells(2))}
    second_slot = {key: slot for slot, key in enumerate(cells(1))}

    def k1(plane, row):
        return first_ref[row_of(first_slot[(plane, row)]), :]

    def k2(plane, row):
        return second_ref[row_of(second_slot[(plane, row)]), :]

    def apply(field, plane, row):
        center = field(plane, row)
        beside = field(plane - 1, row) + field(plane + 1, row)
        beside = beside + (field(plane, row - 1) + field(plane, row + 1))
        beside = beside + (pltpu.roll(center, 1, 1) + pltpu.roll(center, LANES - 1, 1))
        return factor(plane, row) * center - beside

    def keep(order, plane, row, value):
        columns = pl.ds((plane * ROWS + row) * LANES, LANES)
        upper = value.astype(BF16)
        high_out[row_of(order), columns] = upper
        if order == 0:
            low_out[row_of(order), columns] = jnp.zeros_like(upper)
        else:
            low_out[row_of(order), columns] = (value - upper.astype(F32)).astype(BF16)

    for plane, row in cells(0):
        keep(0, plane, row, k0(plane, row))
    for plane, row in cells(2):
        value = apply(k0, plane, row)
        first_ref[row_of(first_slot[(plane, row)]), :] = value
        if distance(plane) == 0 and 0 <= row < ROWS:
            keep(1, plane, row, value)
    for plane, row in cells(1):
        value = apply(k1, plane, row) - B0 * k0(plane, row)
        second_ref[row_of(second_slot[(plane, row)]), :] = value
        if distance(plane) == 0 and 0 <= row < ROWS:
            keep(2, plane, row, value)
    for plane, row in cells(0):
        keep(3, plane, row, apply(k2, plane, row) - B1 * k1(plane, row))
    upper = high_out[...]
    lower = low_out[...]
    top = nt_dot(upper[:PROBES], upper) + nt_dot(upper[:PROBES], lower)
    bottom = nt_dot(upper[3 * PROBES :], upper) + nt_dot(upper[3 * PROBES :], lower)
    gram_ref[:PROBES, :] = top
    gram_ref[PROBES:, :] = bottom + nt_dot(lower[3 * PROBES :], upper)


def basis(*operands):
    width = CELLS * LANES
    return pl.pallas_call(
        basis_kernel,
        out_shape=(
            shaped(4 * PROBES, width, dtype=BF16),
            shaped(4 * PROBES, width, dtype=BF16),
            shaped(2 * PROBES, LANES),
        ),
        in_specs=vmem_specs(len(operands)),
        out_specs=tuple(vmem_specs(3)),
        scratch_shapes=[pltpu.VMEM((108 * PROBES, LANES), F32), pltpu.VMEM((68 * PROBES, LANES), F32)],
        compiler_params=pltpu.CompilerParams(vmem_limit_bytes=VMEM_LIMIT),
        interpret=INTERPRET,
        name="basis",
    )(*held(*operands))


def eliminate(system, block):
    groups = PROBES // 8
    lane = lax.broadcasted_iota(jnp.int32, (8, LANES), 1)
    sub = lax.broadcasted_iota(jnp.int32, (8, LANES), 0)
    start = block * PROBES
    inside = (lane >= start) & (lane < start + PROBES)
    pivoted = [system[8 * g : 8 * g + 8, :] for g in range(groups)]
    solved = [
        jnp.where(inside, jnp.where(lane - start == sub + 8 * g, 1.0, 0.0), pivoted[g]) for g in range(groups)
    ]
    scales = [None] * PROBES
    for panel in range(0, PROBES, PANEL):
        first_group = panel // 8
        spread = {}
        for k in range(panel, panel + PANEL):
            for g in range(first_group, groups):
                column = pivoted[g][:, start + k : start + k + 1]
                spread[k, g] = jnp.broadcast_to(column, (8, LANES))
        for k in range(panel, panel + PANEL):
            group, line = divmod(k, 8)

            def pivot_row(value):
                return jnp.broadcast_to(value[line : line + 1, :], (8, LANES))

            pivot = pivot_row(spread[k, group])
            inverse = 1.0 / pivot
            scales[k] = lax.rsqrt(pivot)
            multiplier = {}
            for g in range(group, groups):
                value = spread[k, g] * inverse
                if g == group:
                    value = jnp.where(sub > line, value, 0.0)
                multiplier[g] = value
            for other in range(k + 1, panel + PANEL):
                row = pivot_row(spread[other, group])
                for g in range(group, groups):
                    spread[other, g] = spread[other, g] - multiplier[g] * row
            row = pivot_row(pivoted[group])
            solved_row = pivot_row(solved[group])
            for g in range(group, groups):
                pivoted[g] = pivoted[g] - multiplier[g] * row
                solved[g] = solved[g] - multiplier[g] * solved_row
    upper = []
    for g in range(groups):
        scale = scales[8 * g]
        for line in range(1, 8):
            scale = jnp.where(sub == line, scales[8 * g + line], scale)
        solved[g] = solved[g] * scale
        upper.append(jnp.where(inside & (lane - start >= sub + 8 * g), pivoted[g] * scale, 0.0))
    return jnp.concatenate(solved, 0), jnp.concatenate(upper, 0)


def finish_kernel(mirror_ref, gram_ref, high_ref, low_ref, alpha_ref, beta_ref, next_ref):
    exact = lax.Precision.HIGHEST
    lane = lax.broadcasted_iota(jnp.int32, (PROBES, LANES), 1)
    block_of = lane // PROBES
    first = gram_ref[:PROBES, :]
    last = gram_ref[PROBES:, :]

    def moved(value, blocks):
        return pltpu.roll(value, (blocks * PROBES) % LANES, 1)

    second = moved(first, -1) + jnp.where(block_of == 1, B0, B1) * moved(first, 1)
    second = jnp.where(block_of == 3, moved(last, 2), jnp.where(block_of == 0, 0.0, second))
    third = moved(last, 1) + jnp.where(block_of == 2, B1 * moved(second, 1) - B0 * first, 0.0)
    third = jnp.where(block_of < 2, 0.0, third)
    systems = [first, second, third, jnp.where(block_of < 3, 0.0, last)]
    solved = []
    uppers = []
    for block in range(4):
        value, upper = eliminate(systems[block], block)
        solved.append(value)
        uppers.append(upper)
        if block < 3:
            tail = value[:, (block + 1) * PROBES :]
            update = lax.dot_general(
                tail, value, (((0,), (0,)), ((), ())), precision=exact, preferred_element_type=F32
            )
            for later in range(block + 1, 4):
                offset = (later - block - 1) * PROBES
                change = update[offset : offset + PROBES, :]
                change = jnp.where((block_of <= block) | (block_of >= later), change, 0.0)
                systems[later] = systems[later] - change
    weights = solved[3]
    upper = weights.astype(BF16)
    lower = (weights - upper.astype(F32)).astype(BF16)
    high = high_ref[...]
    result = jnp.dot(upper, high, preferred_element_type=F32)
    result = result + jnp.dot(upper, low_ref[...], preferred_element_type=F32)
    result = result + jnp.dot(lower, high, preferred_element_type=F32)
    flip_plane = mirror_ref[0]
    flip_row = mirror_ref[1] * (ROWS - 1)
    for cell in range(CELLS):
        plane, row = divmod(cell, ROWS)
        target = (flip_plane ^ plane) * ROWS + (flip_row ^ row)
        next_ref[pl.ds(target, PROBES, stride=CELLS), :] = result[:, cell * LANES : (cell + 1) * LANES]
    row32 = lax.broadcasted_iota(jnp.int32, (PROBES, PROBES), 0)
    lane32 = lax.broadcasted_iota(jnp.int32, (PROBES, PROBES), 1)
    beta = None
    for block in range(3):
        inverse = jnp.where(block_of == block, solved[block], 0.0)
        alpha = nt_dot(moved(solved[block], -1), inverse, exact)
        if block > 0:
            alpha = alpha - jnp.dot(
                beta, nt_dot(solved[block - 1], inverse, exact), precision=exact, preferred_element_type=F32
            )
        alpha_ref[block] = alpha + jnp.where(row32 == lane32, SHIFT, 0.0)
        beta = nt_dot(moved(uppers[block + 1], -1), inverse, exact)
        beta_ref[block] = jnp.where(row32 <= lane32, beta, 0.0)


def finish(mirror, gram, high, low):
    return pl.pallas_call(
        finish_kernel,
        out_shape=(
            jax.ShapeDtypeStruct((3, PROBES, PROBES), F32),
            jax.ShapeDtypeStruct((3, PROBES, PROBES), F32),
            jax.ShapeDtypeStruct((PROBES * CELLS, LANES), F32),
        ),
        in_specs=[pl.BlockSpec(memory_space=pltpu.SMEM)] + vmem_specs(3),
        out_specs=tuple(vmem_specs(3)),
        compiler_params=pltpu.CompilerParams(vmem_limit_bytes=VMEM_LIMIT),
        interpret=INTERPRET,
        name="finish",
    )(mirror, *held(gram, high, low))


def off_chip(x):
    count = lax.axis_size(GX)
    return lax.ppermute(x, GX, [(i, (i - 1 if i % 2 == 0 else i + 1) % count) for i in range(count)])


def same_core(x):
    count = lax.axis_size(GX)
    return lax.ppermute(x, GX, [(i, (i + 2 if i % 2 == 0 else i - 2) % count) for i in range(count)])


def on_chip(x):
    count = lax.axis_size(CORE)
    return lax.ppermute(x, CORE, [(i, count - 1 - i) for i in range(count)])


def row_pair(x, offset):
    count = lax.axis_size(GY)
    step = lambda i: i + 1 if i % 2 == offset else i - 1
    return lax.ppermute(x, GY, [(i, step(i) % count) for i in range(count)])


def exchanged(x, axes):
    return lax.all_to_all(x, axes, 0, 0, tiled=True)


def gathered(x, axes):
    return exchanged(jnp.broadcast_to(x[None], (lax.axis_size(axes),) + x.shape), axes)


def reduced(x):
    near = lax.axis_size(NEAR)
    part = exchanged(x.reshape(near, x.shape[0] // near, x.shape[1]), NEAR).sum(0)
    part = gathered(part, FAR).sum(0)
    return gathered(part, NEAR).reshape(x.shape)


def per_device(probe_signs, diagonal):
    signs = probe_signs.reshape(PROBES * CELLS, LANES)
    diag = diagonal.reshape(CELLS, LANES)
    mirror = jnp.stack([lax.axis_index(CORE), lax.axis_index("gy_1")]).astype(jnp.int32)
    own, outer, top, bottom = prepare(mirror, signs, diag)
    near = off_chip(own)
    high = row_pair(top, 0)
    low = row_pair(bottom, 1)
    far = same_core(outer)
    beside = on_chip(own)
    corner_message, cross_message = pack(high, low, near)
    corner = off_chip(corner_message)
    cross = on_chip(cross_message)
    upper, lower, gram = basis(own, high, low, near, beside, far, corner, cross)
    alphas, betas, following = finish(mirror, reduced(gram), upper, lower)
    return (alphas, betas, following.reshape(PROBES, PLANES, ROWS, LANES))


def solution(mesh):
    split = Mesh(mesh.devices.reshape(2, 8, 2, 8, 2), ("gx_0", "gx_1", "gx_2", "gy_0", "gy_1"))
    placed = (P(None, GX, GY, None), P(GX, GY, None))
    return jax.shard_map(
        per_device,
        mesh=split,
        in_specs=placed,
        out_specs=(P(), P(), P(None, GX, GY, None)),
        check_vma=False,
    )
```

```python
import jax
import jax.numpy as jnp
from jax import lax
from jax.experimental import pallas as pl
from jax.experimental.pallas import tpu as pltpu
from jax.sharding import Mesh
from jax.sharding import PartitionSpec as P


GX = ("gx_0", "gx_1", "gx_2")
GY = ("gy_0", "gy_1")
NEAR = ("gx_0", "gx_2", "gy_1")
FAR = ("gx_1", "gy_0")
CORE = "gx_2"

PROBES = 32
LANES = 128
ROWS = 16
PLANES = 2
CELLS = PLANES * ROWS
SHIFT = 7.75
B0 = 7.0
B1 = 10.0
PANEL = 16
F32 = jnp.float32
BF16 = jnp.bfloat16
INTERPRET = False
VMEM_LIMIT = 16 * 2**20

OWN_ROWS = CELLS * PROBES + CELLS
EDGE_ROWS = 2 * 3 * PROBES + 8
CORNER_ROWS = 6 * PROBES + 8
CROSS_ROWS = ROWS * PROBES + CORNER_ROWS


def vmem_specs(count):
    return [pl.BlockSpec(memory_space=pltpu.VMEM) for _ in range(count)]


def shaped(*shape, dtype=F32):
    return pltpu.VMEM(shape, dtype)


def held(*arrays):
    return tuple(pltpu.with_memory_space_constraint(x, pltpu.VMEM) for x in arrays)


def row_of(index):
    return pl.ds(index * PROBES, PROBES)


def prepare_kernel(
    mirror_ref, signs_hbm, diag_hbm, own_ref, far_ref, high_ref, low_ref, signs_ref, diag_ref, arrived
):
    rows = 8 * CELLS
    copies = []
    for group in range(PROBES // 8):
        part = pl.ds(group * rows, rows)
        copies.append(pltpu.make_async_copy(signs_hbm.at[part, :], signs_ref.at[part, :], arrived.at[group]))
    lines = pltpu.make_async_copy(diag_hbm, diag_ref, arrived.at[PROBES // 8])
    lines.start()
    for copy in copies:
        copy.start()
    flip_plane = mirror_ref[0]
    flip_row = mirror_ref[1] * (ROWS - 1)

    def source_of(cell):
        plane, row = divmod(cell, ROWS)
        return (flip_plane ^ plane) * ROWS + (flip_row ^ row)

    lines.wait()
    for cell in range(CELLS):
        plane, row = divmod(cell, ROWS)
        line = diag_ref[pl.ds(source_of(cell), 1), :]
        own_ref[CELLS * PROBES + cell : CELLS * PROBES + cell + 1, :] = line
        for ref, step in ((low_ref, row), (high_ref, ROWS - 1 - row)):
            if step < 2:
                start = 6 * PROBES + plane * 2 + step
                ref[start : start + 1, :] = line
    for ref in (low_ref, high_ref):
        ref[6 * PROBES + 4 :, :] = jnp.zeros((4, LANES), F32)
    for group in range(PROBES // 8):
        copies[group].wait()
        for cell in range(CELLS):
            plane, row = divmod(cell, ROWS)
            bits = signs_ref[pl.ds(group * rows + source_of(cell), 8, stride=CELLS), :]
            probes = (2 * bits - 1).astype(F32)

            def put(ref, index):
                ref[pl.ds(index * PROBES + group * 8, 8), :] = probes

            put(own_ref, cell)
            if plane == 1:
                put(far_ref, row)
            for ref, step in ((low_ref, row), (high_ref, ROWS - 1 - row)):
                if step < 3:
                    put(ref, plane * 3 + step)


def prepare(mirror, signs, diagonal):
    hbm = pl.BlockSpec(memory_space=pltpu.HBM)
    return pl.pallas_call(
        prepare_kernel,
        out_shape=(
            shaped(OWN_ROWS, LANES),
            shaped(ROWS * PROBES, LANES),
            shaped(EDGE_ROWS, LANES),
            shaped(EDGE_ROWS, LANES),
        ),
        in_specs=[pl.BlockSpec(memory_space=pltpu.SMEM), hbm, hbm],
        out_specs=tuple(vmem_specs(4)),
        scratch_shapes=[
            pltpu.VMEM((PROBES * CELLS, LANES), jnp.int32),
            pltpu.VMEM((CELLS, LANES), F32),
            pltpu.SemaphoreType.DMA((PROBES // 8 + 1,)),
        ],
        compiler_params=pltpu.CompilerParams(vmem_limit_bytes=VMEM_LIMIT),
        interpret=INTERPRET,
        name="prepare",
    )(mirror, *(pltpu.with_memory_space_constraint(x, pltpu.HBM) for x in (signs, diagonal)))


def pack_kernel(high_ref, low_ref, near_ref, corner_ref, cross_ref):
    def edge(plane, row):
        if row < 0:
            return low_ref[row_of(plane * 3 - row - 1), :]
        return high_ref[row_of(plane * 3 + row - ROWS), :]

    def edge_line(plane, row):
        ref = low_ref if row < 0 else high_ref
        start = 6 * PROBES + plane * 2
        return ref[start : start + 1, :]

    for row in range(ROWS):
        cross_ref[row_of(row), :] = near_ref[row_of(row), :]
    for ref, plane, first in ((corner_ref, 0, 0), (cross_ref, 1, ROWS)):
        for place, row in enumerate((-2, -1, ROWS, ROWS + 1)):
            ref[row_of(first + place), :] = edge(plane, row)
        for place, row in enumerate((-1, ROWS)):
            ref[row_of(first + 4 + place), :] = edge(1 - plane, row)
            start = (first + 6) * PROBES + place
            ref[start : start + 1, :] = edge_line(plane, row)
        ref[(first + 6) * PROBES + 2 :, :] = jnp.zeros((6, LANES), F32)


def pack(high, low, near):
    return pl.pallas_call(
        pack_kernel,
        out_shape=(shaped(CORNER_ROWS, LANES), shaped(CROSS_ROWS, LANES)),
        in_specs=vmem_specs(3),
        out_specs=tuple(vmem_specs(2)),
        compiler_params=pltpu.CompilerParams(vmem_limit_bytes=VMEM_LIMIT),
        interpret=INTERPRET,
        name="pack",
    )(*held(high, low, near))


def nt_dot(left, right, precision=None):
    return lax.dot_general(
        left, right, (((1,), (1,)), ((), ())), precision=precision, preferred_element_type=F32
    )


def basis_kernel(
    own_ref, high_ref, low_ref, near_ref, beside_ref, far_ref, corner_ref, cross_ref,
    split_out, gram_ref, first_ref, second_ref,
):
    def distance(plane):
        return -plane if plane < 0 else max(plane - (PLANES - 1), 0)

    def k0(plane, row):
        away = distance(plane)
        if away == 0:
            if row < 0:
                return low_ref[row_of(plane * 3 - row - 1), :]
            if row >= ROWS:
                return high_ref[row_of(plane * 3 + row - ROWS), :]
            return own_ref[row_of(plane * ROWS + row), :]
        if away == 3:
            return (far_ref if plane < 0 else cross_ref)[row_of(row), :]
        if 0 <= row < ROWS:
            if plane < 0:
                return near_ref[row_of((away - 1) * ROWS + row), :]
            return beside_ref[row_of((2 - away) * ROWS + row), :]
        ref, first = (corner_ref, 0) if plane < 0 else (cross_ref, ROWS)
        places = (-2, -1, ROWS, ROWS + 1) if away == 1 else (-1, ROWS)
        return ref[row_of(first + 4 * (away - 1) + places.index(row)), :]

    def factor(plane, row):
        away = distance(plane)
        if away == 0:
            if row < 0:
                ref, start = low_ref, 6 * PROBES + plane * 2 - row - 1
            elif row >= ROWS:
                ref, start = high_ref, 6 * PROBES + plane * 2 + row - ROWS
            else:
                ref, start = own_ref, CELLS * PROBES + plane * ROWS + row
        elif 0 <= row < ROWS:
            if plane < 0:
                ref, start = near_ref, CELLS * PROBES + (away - 1) * ROWS + row
            else:
                ref, start = beside_ref, CELLS * PROBES + (2 - away) * ROWS + row
        else:
            ref, first = (corner_ref, 0) if plane < 0 else (cross_ref, ROWS)
            start = (first + 6) * PROBES + (0 if row < 0 else 1)
        return ref[start : start + 1, :] + (6.0 - SHIFT)

    def cells(width):
        found = []
        for plane in range(-width, PLANES + width):
            extra = width - distance(plane)
            for row in range(-extra, ROWS + extra):
                found.append((plane, row))
        return found

    first_slot = {key: slot for slot, key in enumerate(cells(2))}
    second_slot = {key: slot for slot, key in enumerate(cells(1))}

    def k1(plane, row):
        return first_ref[row_of(first_slot[(plane, row)]), :]

    def k2(plane, row):
        return second_ref[row_of(second_slot[(plane, row)]), :]

    def apply(field, plane, row):
        center = field(plane, row)
        beside = field(plane - 1, row) + field(plane + 1, row)
        beside = beside + (field(plane, row - 1) + field(plane, row + 1))
        beside = beside + (pltpu.roll(center, 1, 1) + pltpu.roll(center, LANES - 1, 1))
        return factor(plane, row) * center - beside

    def keep(order, plane, row, value):
        columns = pl.ds((plane * ROWS + row) * LANES, LANES)
        upper = value.astype(BF16)
        split_out[row_of(order), columns] = upper
        if order == 0:
            split_out[row_of(4), columns] = jnp.zeros_like(upper)
        else:
            split_out[row_of(order + 4), columns] = (value - upper.astype(F32)).astype(BF16)

    for plane, row in cells(0):
        keep(0, plane, row, k0(plane, row))
    for plane, row in cells(2):
        value = apply(k0, plane, row)
        first_ref[row_of(first_slot[(plane, row)]), :] = value
        if distance(plane) == 0 and 0 <= row < ROWS:
            keep(1, plane, row, value)
    for plane, row in cells(1):
        value = apply(k1, plane, row) - B0 * k0(plane, row)
        second_ref[row_of(second_slot[(plane, row)]), :] = value
        if distance(plane) == 0 and 0 <= row < ROWS:
            keep(2, plane, row, value)
    for plane, row in cells(0):
        keep(3, plane, row, apply(k2, plane, row) - B1 * k1(plane, row))
    split = split_out[...]
    left = jnp.concatenate([split[:PROBES], split[3 * PROBES : 4 * PROBES], split[7 * PROBES :]], 0)
    product = nt_dot(left, split)
    product = product[:, :LANES] + product[:, LANES:]
    gram_ref[:PROBES, :] = product[:PROBES]
    gram_ref[PROBES:, :] = product[PROBES : 2 * PROBES] + product[2 * PROBES :]


def basis(*operands):
    width = CELLS * LANES
    return pl.pallas_call(
        basis_kernel,
        out_shape=(shaped(8 * PROBES, width, dtype=BF16), shaped(2 * PROBES, LANES)),
        in_specs=vmem_specs(len(operands)),
        out_specs=tuple(vmem_specs(2)),
        scratch_shapes=[pltpu.VMEM((108 * PROBES, LANES), F32), pltpu.VMEM((68 * PROBES, LANES), F32)],
        compiler_params=pltpu.CompilerParams(vmem_limit_bytes=VMEM_LIMIT),
        interpret=INTERPRET,
        name="basis",
    )(*held(*operands))


def eliminate(system, block):
    groups = PROBES // 8
    lane = lax.broadcasted_iota(jnp.int32, (8, LANES), 1)
    sub = lax.broadcasted_iota(jnp.int32, (8, LANES), 0)
    start = block * PROBES
    inside = (lane >= start) & (lane < start + PROBES)
    pivoted = [system[8 * g : 8 * g + 8, :] for g in range(groups)]
    solved = [
        jnp.where(inside, jnp.where(lane - start == sub + 8 * g, 1.0, 0.0), pivoted[g]) for g in range(groups)
    ]
    scales = [None] * PROBES
    for panel in range(0, PROBES, PANEL):
        first_group = panel // 8
        spread = {}
        for k in range(panel, panel + PANEL):
            for g in range(first_group, groups):
                column = pivoted[g][:, start + k : start + k + 1]
                spread[k, g] = jnp.broadcast_to(column, (8, LANES))
        for k in range(panel, panel + PANEL):
            group, line = divmod(k, 8)

            def pivot_row(value):
                return jnp.broadcast_to(value[line : line + 1, :], (8, LANES))

            pivot = pivot_row(spread[k, group])
            inverse = 1.0 / pivot
            scales[k] = lax.rsqrt(pivot)
            multiplier = {}
            for g in range(group, groups):
                value = spread[k, g] * inverse
                if g == group:
                    value = jnp.where(sub > line, value, 0.0)
                multiplier[g] = value
            for other in range(k + 1, panel + PANEL):
                row = pivot_row(spread[other, group])
                for g in range(group, groups):
                    spread[other, g] = spread[other, g] - multiplier[g] * row
            row = pivot_row(pivoted[group])
            solved_row = pivot_row(solved[group])
            for g in range(group, groups):
                pivoted[g] = pivoted[g] - multiplier[g] * row
                solved[g] = solved[g] - multiplier[g] * solved_row
    upper = []
    for g in range(groups):
        scale = scales[8 * g]
        for line in range(1, 8):
            scale = jnp.where(sub == line, scales[8 * g + line], scale)
        solved[g] = solved[g] * scale
        upper.append(jnp.where(inside & (lane - start >= sub + 8 * g), pivoted[g] * scale, 0.0))
    return jnp.concatenate(solved, 0), jnp.concatenate(upper, 0)


def parts_of(value):
    upper = value.astype(BF16)
    rest = value - upper.astype(F32)
    middle = rest.astype(BF16)
    return upper, middle, (rest - middle.astype(F32)).astype(BF16)


def square(value):
    upper, middle, lower = parts_of(value)
    left = jnp.concatenate([upper, upper, middle, middle, upper, lower], 0)
    right = jnp.concatenate([upper, middle, upper, middle, lower, upper], 0)
    return lax.dot_general(left, right, (((0,), (0,)), ((), ())), preferred_element_type=F32)


def finish_kernel(mirror_ref, gram_ref, split_ref, alpha_ref, beta_ref, next_ref):
    exact = lax.Precision.HIGHEST
    lane = lax.broadcasted_iota(jnp.int32, (PROBES, LANES), 1)
    block_of = lane // PROBES
    first = gram_ref[:PROBES, :]
    last = gram_ref[PROBES:, :]

    def moved(value, blocks):
        return pltpu.roll(value, (blocks * PROBES) % LANES, 1)

    second = moved(first, -1) + jnp.where(block_of == 1, B0, B1) * moved(first, 1)
    second = jnp.where(block_of == 3, moved(last, 2), jnp.where(block_of == 0, 0.0, second))
    third = moved(last, 1) + jnp.where(block_of == 2, B1 * moved(second, 1) - B0 * first, 0.0)
    third = jnp.where(block_of < 2, 0.0, third)
    systems = [first, second, third, jnp.where(block_of < 3, 0.0, last)]
    solved = []
    uppers = []
    for block in range(4):
        value, upper = eliminate(systems[block], block)
        solved.append(value)
        uppers.append(upper)
        if block < 3:
            update = square(value)
            for later in range(block + 1, 4):
                change = update[later * PROBES : (later + 1) * PROBES, :]
                change = jnp.where((block_of <= block) | (block_of >= later), change, 0.0)
                systems[later] = systems[later] - change
    upper, lower, _ = parts_of(solved[3])
    weights = jnp.concatenate(
        [jnp.concatenate([upper, upper], 1), jnp.concatenate([lower, jnp.zeros_like(lower)], 1)], 0
    )
    result = jnp.dot(weights, split_ref[...], preferred_element_type=F32)
    result = result[:PROBES] + result[PROBES:]
    flip_plane = mirror_ref[0]
    flip_row = mirror_ref[1] * (ROWS - 1)
    for cell in range(CELLS):
        plane, row = divmod(cell, ROWS)
        target = (flip_plane ^ plane) * ROWS + (flip_row ^ row)
        next_ref[pl.ds(target, PROBES, stride=CELLS), :] = result[:, cell * LANES : (cell + 1) * LANES]
    row32 = lax.broadcasted_iota(jnp.int32, (PROBES, PROBES), 0)
    lane32 = lax.broadcasted_iota(jnp.int32, (PROBES, PROBES), 1)
    beta = None
    for block in range(3):
        inverse = jnp.where(block_of == block, solved[block], 0.0)
        alpha = nt_dot(moved(solved[block], -1), inverse, exact)
        if block > 0:
            alpha = alpha - jnp.dot(
                beta, nt_dot(solved[block - 1], inverse, exact), precision=exact, preferred_element_type=F32
            )
        alpha_ref[block] = alpha + jnp.where(row32 == lane32, SHIFT, 0.0)
        beta = nt_dot(moved(uppers[block + 1], -1), inverse, exact)
        beta_ref[block] = jnp.where(row32 <= lane32, beta, 0.0)


def finish(mirror, gram, split):
    return pl.pallas_call(
        finish_kernel,
        out_shape=(
            jax.ShapeDtypeStruct((3, PROBES, PROBES), F32),
            jax.ShapeDtypeStruct((3, PROBES, PROBES), F32),
            jax.ShapeDtypeStruct((PROBES * CELLS, LANES), F32),
        ),
        in_specs=[pl.BlockSpec(memory_space=pltpu.SMEM)] + vmem_specs(2),
        out_specs=tuple(vmem_specs(3)),
        compiler_params=pltpu.CompilerParams(vmem_limit_bytes=VMEM_LIMIT),
        interpret=INTERPRET,
        name="finish",
    )(mirror, *held(gram, split))


def off_chip(x):
    count = lax.axis_size(GX)
    return lax.ppermute(x, GX, [(i, (i - 1 if i % 2 == 0 else i + 1) % count) for i in range(count)])


def same_core(x):
    count = lax.axis_size(GX)
    return lax.ppermute(x, GX, [(i, (i + 2 if i % 2 == 0 else i - 2) % count) for i in range(count)])


def on_chip(x):
    count = lax.axis_size(CORE)
    return lax.ppermute(x, CORE, [(i, count - 1 - i) for i in range(count)])


def row_pair(x, offset):
    count = lax.axis_size(GY)
    step = lambda i: i + 1 if i % 2 == offset else i - 1
    return lax.ppermute(x, GY, [(i, step(i) % count) for i in range(count)])


def exchanged(x, axes):
    return lax.all_to_all(x, axes, 0, 0, tiled=True)


def gathered(x, axes):
    return exchanged(jnp.broadcast_to(x[None], (lax.axis_size(axes),) + x.shape), axes)


def reduced(x):
    near = lax.axis_size(NEAR)
    part = exchanged(x.reshape(near, x.shape[0] // near, x.shape[1]), NEAR).sum(0)
    part = gathered(part, FAR).sum(0)
    return gathered(part, NEAR).reshape(x.shape)


def per_device(probe_signs, diagonal):
    signs = probe_signs.reshape(PROBES * CELLS, LANES)
    diag = diagonal.reshape(CELLS, LANES)
    mirror = jnp.stack([lax.axis_index(CORE), lax.axis_index("gy_1")]).astype(jnp.int32)
    own, outer, top, bottom = prepare(mirror, signs, diag)
    near = off_chip(own)
    high = row_pair(top, 0)
    low = row_pair(bottom, 1)
    far = same_core(outer)
    beside = on_chip(own)
    corner_message, cross_message = pack(high, low, near)
    corner = off_chip(corner_message)
    cross = on_chip(cross_message)
    split, gram = basis(own, high, low, near, beside, far, corner, cross)
    alphas, betas, following = finish(mirror, reduced(gram), split)
    return (alphas, betas, following.reshape(PROBES, PLANES, ROWS, LANES))


def solution(mesh):
    split = Mesh(mesh.devices.reshape(2, 8, 2, 8, 2), ("gx_0", "gx_1", "gx_2", "gy_0", "gy_1"))
    placed = (P(None, GX, GY, None), P(GX, GY, None))
    return jax.shard_map(
        per_device,
        mesh=split,
        in_specs=placed,
        out_specs=(P(), P(), P(None, GX, GY, None)),
        check_vma=False,
    )
```

```python
import jax
import jax.numpy as jnp
from jax import lax
from jax.experimental import pallas as pl
from jax.experimental.pallas import tpu as pltpu
from jax.sharding import Mesh
from jax.sharding import PartitionSpec as P


GX = ("gx_0", "gx_1", "gx_2")
GY = ("gy_0", "gy_1")
NEAR = ("gx_0", "gx_2", "gy_1")
FAR = ("gx_1", "gy_0")
CORE = "gx_2"
PAIR = "gy_1"

PROBES = 32
LANES = 128
ROWS = 16
PLANES = 2
CELLS = PLANES * ROWS
SHIFT = 7.75
B0 = 7.0
B1 = 10.0
PANEL = 8
F32 = jnp.float32
BF16 = jnp.bfloat16
INTERPRET = False
VMEM_LIMIT = 16 * 2**20

OWN_ROWS = CELLS * PROBES + CELLS
EDGE_ROWS = 2 * 3 * PROBES + 8
CORNER_ROWS = 6 * PROBES + 8
CROSS_ROWS = ROWS * PROBES + CORNER_ROWS


def vmem_specs(count):
    return [pl.BlockSpec(memory_space=pltpu.VMEM) for _ in range(count)]


def shaped(*shape, dtype=F32):
    return pltpu.VMEM(shape, dtype)


def held(*arrays):
    return tuple(pltpu.with_memory_space_constraint(x, pltpu.VMEM) for x in arrays)


def row_of(index):
    return pl.ds(index * PROBES, PROBES)


def mirrored():
    core = lax.axis_index(CORE)
    pair = lax.axis_index(PAIR)

    def position(plane, row):
        return (plane + core * (1 - 2 * plane)) * ROWS + row + pair * (ROWS - 1 - 2 * row)

    return position


def prepare_kernel(
    signs_hbm, diag_hbm, own_ref, far_ref, high_ref, low_ref, signs_ref, diag_ref, arrived
):
    rows = 8 * CELLS
    copies = []
    for group in range(PROBES // 8):
        part = pl.ds(group * rows, rows)
        copies.append(pltpu.make_async_copy(signs_hbm.at[part, :], signs_ref.at[part, :], arrived.at[group]))
    lines = pltpu.make_async_copy(diag_hbm, diag_ref, arrived.at[PROBES // 8])
    lines.start()
    for copy in copies:
        copy.start()
    position = mirrored()

    lines.wait()
    for cell in range(CELLS):
        plane, row = divmod(cell, ROWS)
        line = diag_ref[pl.ds(position(plane, row), 1), :]
        own_ref[CELLS * PROBES + cell : CELLS * PROBES + cell + 1, :] = line
        for ref, step in ((low_ref, row), (high_ref, ROWS - 1 - row)):
            if step < 2:
                start = 6 * PROBES + plane * 2 + step
                ref[start : start + 1, :] = line
    for ref in (low_ref, high_ref):
        ref[6 * PROBES + 4 :, :] = jnp.zeros((4, LANES), F32)
    for group in range(PROBES // 8):
        copies[group].wait()
        for cell in range(CELLS):
            plane, row = divmod(cell, ROWS)
            bits = signs_ref[pl.ds(group * rows + position(plane, row), 8, stride=CELLS), :]
            probes = (2 * bits - 1).astype(F32)

            def put(ref, index):
                ref[pl.ds(index * PROBES + group * 8, 8), :] = probes

            put(own_ref, cell)
            if plane == 1:
                put(far_ref, row)
            for ref, step in ((low_ref, row), (high_ref, ROWS - 1 - row)):
                if step < 3:
                    put(ref, plane * 3 + step)


def prepare(signs, diagonal):
    hbm = pl.BlockSpec(memory_space=pltpu.HBM)
    return pl.pallas_call(
        prepare_kernel,
        out_shape=(
            shaped(OWN_ROWS, LANES),
            shaped(ROWS * PROBES, LANES),
            shaped(EDGE_ROWS, LANES),
            shaped(EDGE_ROWS, LANES),
        ),
        in_specs=[hbm, hbm],
        out_specs=tuple(vmem_specs(4)),
        scratch_shapes=[
            pltpu.VMEM((PROBES * CELLS, LANES), jnp.int32),
            pltpu.VMEM((CELLS, LANES), F32),
            pltpu.SemaphoreType.DMA((PROBES // 8 + 1,)),
        ],
        compiler_params=pltpu.CompilerParams(vmem_limit_bytes=VMEM_LIMIT),
        interpret=INTERPRET,
        name="prepare",
    )(*(pltpu.with_memory_space_constraint(x, pltpu.HBM) for x in (signs, diagonal)))


def pack_kernel(high_ref, low_ref, near_ref, corner_ref, cross_ref):
    def edge(plane, row):
        if row < 0:
            return low_ref[row_of(plane * 3 - row - 1), :]
        return high_ref[row_of(plane * 3 + row - ROWS), :]

    def edge_line(plane, row):
        ref = low_ref if row < 0 else high_ref
        start = 6 * PROBES + plane * 2
        return ref[start : start + 1, :]

    for row in range(ROWS):
        cross_ref[row_of(row), :] = near_ref[row_of(row), :]
    for ref, plane, first in ((corner_ref, 0, 0), (cross_ref, 1, ROWS)):
        for place, row in enumerate((-2, -1, ROWS, ROWS + 1)):
            ref[row_of(first + place), :] = edge(plane, row)
        for place, row in enumerate((-1, ROWS)):
            ref[row_of(first + 4 + place), :] = edge(1 - plane, row)
            start = (first + 6) * PROBES + place
            ref[start : start + 1, :] = edge_line(plane, row)
        ref[(first + 6) * PROBES + 2 :, :] = jnp.zeros((6, LANES), F32)


def pack(high, low, near):
    return pl.pallas_call(
        pack_kernel,
        out_shape=(shaped(CORNER_ROWS, LANES), shaped(CROSS_ROWS, LANES)),
        in_specs=vmem_specs(3),
        out_specs=tuple(vmem_specs(2)),
        compiler_params=pltpu.CompilerParams(vmem_limit_bytes=VMEM_LIMIT),
        interpret=INTERPRET,
        name="pack",
    )(*held(high, low, near))


def nt_dot(left, right):
    return lax.dot_general(left, right, (((1,), (1,)), ((), ())), preferred_element_type=F32)


def basis_kernel(
    own_ref, high_ref, low_ref, near_ref, beside_ref, far_ref, corner_ref, cross_ref,
    split_out, gram_ref, first_ref, second_ref,
):
    def distance(plane):
        return -plane if plane < 0 else max(plane - (PLANES - 1), 0)

    def k0(plane, row):
        away = distance(plane)
        if away == 0:
            if row < 0:
                return low_ref[row_of(plane * 3 - row - 1), :]
            if row >= ROWS:
                return high_ref[row_of(plane * 3 + row - ROWS), :]
            return own_ref[row_of(plane * ROWS + row), :]
        if away == 3:
            return (far_ref if plane < 0 else cross_ref)[row_of(row), :]
        if 0 <= row < ROWS:
            if plane < 0:
                return near_ref[row_of((away - 1) * ROWS + row), :]
            return beside_ref[row_of((2 - away) * ROWS + row), :]
        ref, first = (corner_ref, 0) if plane < 0 else (cross_ref, ROWS)
        places = (-2, -1, ROWS, ROWS + 1) if away == 1 else (-1, ROWS)
        return ref[row_of(first + 4 * (away - 1) + places.index(row)), :]

    def factor(plane, row):
        away = distance(plane)
        if away == 0:
            if row < 0:
                ref, start = low_ref, 6 * PROBES + plane * 2 - row - 1
            elif row >= ROWS:
                ref, start = high_ref, 6 * PROBES + plane * 2 + row - ROWS
            else:
                ref, start = own_ref, CELLS * PROBES + plane * ROWS + row
        elif 0 <= row < ROWS:
            if plane < 0:
                ref, start = near_ref, CELLS * PROBES + (away - 1) * ROWS + row
            else:
                ref, start = beside_ref, CELLS * PROBES + (2 - away) * ROWS + row
        else:
            ref, first = (corner_ref, 0) if plane < 0 else (cross_ref, ROWS)
            start = (first + 6) * PROBES + (0 if row < 0 else 1)
        return ref[start : start + 1, :] + (6.0 - SHIFT)

    def cells(width):
        found = []
        for plane in range(-width, PLANES + width):
            extra = width - distance(plane)
            for row in range(-extra, ROWS + extra):
                found.append((plane, row))
        return found

    first_slot = {key: slot for slot, key in enumerate(cells(2))}
    second_slot = {key: slot for slot, key in enumerate(cells(1))}

    def k1(plane, row):
        return first_ref[row_of(first_slot[(plane, row)]), :]

    def k2(plane, row):
        return second_ref[row_of(second_slot[(plane, row)]), :]

    def apply(field, plane, row):
        center = field(plane, row)
        beside = field(plane - 1, row) + field(plane + 1, row)
        beside = beside + (field(plane, row - 1) + field(plane, row + 1))
        beside = beside + (pltpu.roll(center, 1, 1) + pltpu.roll(center, LANES - 1, 1))
        return factor(plane, row) * center - beside

    def keep(order, plane, row, value):
        columns = pl.ds((plane * ROWS + row) * LANES, LANES)
        upper = value.astype(BF16)
        split_out[row_of(order), columns] = upper
        if order == 0:
            split_out[row_of(4), columns] = jnp.zeros_like(upper)
        else:
            split_out[row_of(order + 4), columns] = (value - upper.astype(F32)).astype(BF16)

    for plane, row in cells(0):
        keep(0, plane, row, k0(plane, row))
    for plane, row in cells(2):
        value = apply(k0, plane, row)
        first_ref[row_of(first_slot[(plane, row)]), :] = value
        if distance(plane) == 0 and 0 <= row < ROWS:
            keep(1, plane, row, value)
    for plane, row in cells(1):
        value = apply(k1, plane, row) - B0 * k0(plane, row)
        second_ref[row_of(second_slot[(plane, row)]), :] = value
        if distance(plane) == 0 and 0 <= row < ROWS:
            keep(2, plane, row, value)
    for plane, row in cells(0):
        keep(3, plane, row, apply(k2, plane, row) - B1 * k1(plane, row))
    split = split_out[...]
    left = jnp.concatenate([split[:PROBES], split[3 * PROBES : 4 * PROBES], split[7 * PROBES :]], 0)
    product = nt_dot(left, split)
    product = product[:, :LANES] + product[:, LANES:]
    gram_ref[:PROBES, :] = product[:PROBES]
    gram_ref[PROBES:, :] = product[PROBES : 2 * PROBES] + product[2 * PROBES :]


def basis(*operands):
    width = CELLS * LANES
    return pl.pallas_call(
        basis_kernel,
        out_shape=(shaped(8 * PROBES, width, dtype=BF16), shaped(2 * PROBES, LANES)),
        in_specs=vmem_specs(len(operands)),
        out_specs=tuple(vmem_specs(2)),
        scratch_shapes=[pltpu.VMEM((108 * PROBES, LANES), F32), pltpu.VMEM((68 * PROBES, LANES), F32)],
        compiler_params=pltpu.CompilerParams(vmem_limit_bytes=VMEM_LIMIT),
        interpret=INTERPRET,
        name="basis",
    )(*held(*operands))


def eliminate(system, block):
    groups = PROBES // 8
    lane = lax.broadcasted_iota(jnp.int32, (8, LANES), 1)
    sub = lax.broadcasted_iota(jnp.int32, (8, LANES), 0)
    start = block * PROBES
    inside = (lane >= start) & (lane < start + PROBES)
    pivoted = [system[8 * g : 8 * g + 8, :] for g in range(groups)]
    solved = [
        jnp.where(inside, jnp.where(lane - start == sub + 8 * g, 1.0, 0.0), pivoted[g]) for g in range(groups)
    ]
    scales = [None] * PROBES
    spread = {}

    def spread_panel(panel):
        for k in range(panel, min(panel + PANEL, PROBES)):
            for g in range(max(panel - PANEL, 0) // 8, groups):
                column = pivoted[g][:, start + k : start + k + 1]
                spread[k, g] = jnp.broadcast_to(column, (8, LANES))

    spread_panel(0)
    for panel in range(0, PROBES, PANEL):
        spread_panel(panel + PANEL)
        for k in range(panel, panel + PANEL):
            group, line = divmod(k, 8)

            def pivot_row(value):
                return jnp.broadcast_to(value[line : line + 1, :], (8, LANES))

            pivot = pivot_row(spread[k, group])
            inverse = 1.0 / pivot
            scales[k] = lax.rsqrt(pivot)
            multiplier = {}
            for g in range(group, groups):
                value = spread[k, g] * inverse
                if g == group:
                    value = jnp.where(sub > line, value, 0.0)
                multiplier[g] = value
            row = pivot_row(pivoted[group])
            solved_row = pivot_row(solved[group])
            for other in range(k + 1, min(panel + 2 * PANEL, PROBES)):
                weight = pivot_row(spread[other, group])
                for g in range(group, groups):
                    spread[other, g] = spread[other, g] - multiplier[g] * weight
            for g in range(group, groups):
                pivoted[g] = pivoted[g] - multiplier[g] * row
                solved[g] = solved[g] - multiplier[g] * solved_row
    upper = []
    for g in range(groups):
        scale = scales[8 * g]
        for line in range(1, 8):
            scale = jnp.where(sub == line, scales[8 * g + line], scale)
        solved[g] = solved[g] * scale
        upper.append(jnp.where(inside & (lane - start >= sub + 8 * g), pivoted[g] * scale, 0.0))
    return jnp.concatenate(solved, 0), jnp.concatenate(upper, 0)


def parts_of(value):
    upper = value.astype(BF16)
    rest = value - upper.astype(F32)
    middle = rest.astype(BF16)
    return upper, middle, (rest - middle.astype(F32)).astype(BF16)


def square(value):
    upper, middle, lower = parts_of(value)
    left = jnp.concatenate([upper, upper, middle, middle, upper, lower], 0)
    right = jnp.concatenate([upper, middle, upper, middle, lower, upper], 0)
    return lax.dot_general(left, right, (((0,), (0,)), ((), ())), preferred_element_type=F32)


def wide_dot(left, right):
    left_upper, left_lower, _ = parts_of(left)
    right_upper, right_lower, _ = parts_of(right)
    both = jnp.concatenate([left_upper, left_lower], 1)
    result = nt_dot(both, jnp.concatenate([right_upper, right_upper], 1))
    return result + nt_dot(both, jnp.concatenate([right_lower, right_lower], 1))


def finish_kernel(gram_ref, split_ref, alpha_ref, beta_ref, next_hbm, next_ref, left):
    lane = lax.broadcasted_iota(jnp.int32, (PROBES, LANES), 1)
    block_of = lane // PROBES
    first = gram_ref[:PROBES, :]
    last = gram_ref[PROBES:, :]

    def moved(value, blocks):
        return pltpu.roll(value, (blocks * PROBES) % LANES, 1)

    second = moved(first, -1) + jnp.where(block_of == 1, B0, B1) * moved(first, 1)
    second = jnp.where(block_of == 3, moved(last, 2), jnp.where(block_of == 0, 0.0, second))
    third = moved(last, 1) + jnp.where(block_of == 2, B1 * moved(second, 1) - B0 * first, 0.0)
    third = jnp.where(block_of < 2, 0.0, third)
    systems = [first, second, third, jnp.where(block_of < 3, 0.0, last)]
    row32 = lax.broadcasted_iota(jnp.int32, (PROBES, PROBES), 0)
    lane32 = lax.broadcasted_iota(jnp.int32, (PROBES, PROBES), 1)
    solved = []
    beta = None
    for block in range(4):
        value, triangle = eliminate(systems[block], block)
        solved.append(value)
        if block < 3:
            update = square(value)
            for later in range(block + 1, 4):
                change = update[later * PROBES : (later + 1) * PROBES, :]
                change = jnp.where((block_of <= block) | (block_of >= later), change, 0.0)
                systems[later] = systems[later] - change
        if block > 0:
            beta = wide_dot(moved(triangle, -1), inverse)
            beta_ref[block - 1] = jnp.where(row32 <= lane32, beta, 0.0)
        if block < 3:
            inverse = jnp.where(block_of == block, value, 0.0)
            alpha = wide_dot(moved(value, -1), inverse)
            if block > 0:
                coupled = wide_dot(solved[block - 1], inverse)
                alpha = alpha - jnp.dot(
                    beta, coupled, precision=lax.Precision.HIGHEST, preferred_element_type=F32
                )
            alpha_ref[block] = alpha + jnp.where(row32 == lane32, SHIFT, 0.0)
    upper, lower, _ = parts_of(solved[3])
    weights = jnp.concatenate(
        [jnp.concatenate([upper, upper], 1), jnp.concatenate([lower, jnp.zeros_like(lower)], 1)], 0
    )
    position = mirrored()
    view = next_ref.reshape(PROBES, CELLS, LANES)
    copies = []
    for group in range(CELLS // 8):
        columns = pl.ds(group * 8 * LANES, 8 * LANES)
        result = jnp.dot(weights, split_ref[:, columns], preferred_element_type=F32)
        result = result[:PROBES] + result[PROBES:]
        for place in range(8):
            plane, row = divmod(group * 8 + place, ROWS)
            target = pl.ds(position(plane, row), PROBES, stride=CELLS)
            next_ref[target, :] = result[:, place * LANES : (place + 1) * LANES]
        plane, half = divmod(group, 2)
        core, pair = lax.axis_index(CORE), lax.axis_index(PAIR)
        first = (plane + core * (1 - 2 * plane)) * ROWS + (half + pair * (1 - 2 * half)) * 8
        part = pl.ds(pl.multiple_of(first, 8), 8)
        copy = pltpu.make_async_copy(view.at[:, part, :], next_hbm.at[:, part, :], left.at[group])
        copy.start()
        copies.append(copy)
    for copy in copies:
        copy.wait()


def finish(gram, split):
    return pl.pallas_call(
        finish_kernel,
        out_shape=(
            jax.ShapeDtypeStruct((3, PROBES, PROBES), F32),
            jax.ShapeDtypeStruct((3, PROBES, PROBES), F32),
            jax.ShapeDtypeStruct((PROBES, CELLS, LANES), F32),
        ),
        in_specs=vmem_specs(2),
        out_specs=tuple(vmem_specs(2)) + (pl.BlockSpec(memory_space=pltpu.HBM),),
        scratch_shapes=[
            pltpu.VMEM((PROBES * CELLS, LANES), F32),
            pltpu.SemaphoreType.DMA((CELLS // 8,)),
        ],
        compiler_params=pltpu.CompilerParams(vmem_limit_bytes=VMEM_LIMIT),
        interpret=INTERPRET,
        name="finish",
    )(*held(gram, split))


def off_chip(x):
    count = lax.axis_size(GX)
    return lax.ppermute(x, GX, [(i, (i - 1 if i % 2 == 0 else i + 1) % count) for i in range(count)])


def same_core(x):
    count = lax.axis_size(GX)
    return lax.ppermute(x, GX, [(i, (i + 2 if i % 2 == 0 else i - 2) % count) for i in range(count)])


def on_chip(x):
    count = lax.axis_size(CORE)
    return lax.ppermute(x, CORE, [(i, count - 1 - i) for i in range(count)])


def row_pair(x, offset):
    count = lax.axis_size(GY)
    step = lambda i: i + 1 if i % 2 == offset else i - 1
    return lax.ppermute(x, GY, [(i, step(i) % count) for i in range(count)])


def exchanged(x, axes):
    return lax.all_to_all(x, axes, 0, 0, tiled=True)


def gathered(x, axes):
    return exchanged(jnp.broadcast_to(x[None], (lax.axis_size(axes),) + x.shape), axes)


def reduced(x):
    near = lax.axis_size(NEAR)
    part = exchanged(x.reshape(near, x.shape[0] // near, x.shape[1]), NEAR).sum(0)
    part = gathered(part, FAR).sum(0)
    return gathered(part, NEAR).reshape(x.shape)


def per_device(probe_signs, diagonal):
    signs = probe_signs.reshape(PROBES * CELLS, LANES)
    diag = diagonal.reshape(CELLS, LANES)
    own, outer, top, bottom = prepare(signs, diag)
    near = off_chip(own)
    high = row_pair(top, 0)
    low = row_pair(bottom, 1)
    far = same_core(outer)
    beside = on_chip(own)
    corner_message, cross_message = pack(high, low, near)
    corner = off_chip(corner_message)
    cross = on_chip(cross_message)
    split, gram = basis(own, high, low, near, beside, far, corner, cross)
    alphas, betas, following = finish(reduced(gram), split)
    return (alphas, betas, following.reshape(PROBES, PLANES, ROWS, LANES))


def solution(mesh):
    split = Mesh(mesh.devices.reshape(2, 8, 2, 8, 2), ("gx_0", "gx_1", "gx_2", "gy_0", "gy_1"))
    placed = (P(None, GX, GY, None), P(GX, GY, None))
    return jax.shard_map(
        per_device,
        mesh=split,
        in_specs=placed,
        out_specs=(P(), P(), P(None, GX, GY, None)),
        check_vma=False,
    )
```

```python
import jax
import jax.numpy as jnp
from jax import lax
from jax.experimental import pallas as pl
from jax.experimental.pallas import tpu as pltpu
from jax.sharding import Mesh
from jax.sharding import PartitionSpec as P


GX = ("gx_0", "gx_1", "gx_2")
GY = ("gy_0", "gy_1")
NEAR = ("gx_0", "gx_2", "gy_1")
FAR = ("gx_1", "gy_0")
CORE = "gx_2"
PAIR = "gy_1"

PROBES = 32
LANES = 128
ROWS = 16
PLANES = 2
CELLS = PLANES * ROWS
SHIFT = 7.75
B0 = 7.0
B1 = 10.0
PANEL = 8
F32 = jnp.float32
BF16 = jnp.bfloat16
INTERPRET = False
VMEM_LIMIT = 16 * 2**20

OWN_ROWS = CELLS * PROBES + CELLS
EDGE_ROWS = 2 * 3 * PROBES + 8
CORNER_ROWS = 6 * PROBES + 8
CROSS_ROWS = ROWS * PROBES + CORNER_ROWS


def vmem_specs(count):
    return [pl.BlockSpec(memory_space=pltpu.VMEM) for _ in range(count)]


def shaped(*shape, dtype=F32):
    return pltpu.VMEM(shape, dtype)


def held(*arrays):
    return tuple(pltpu.with_memory_space_constraint(x, pltpu.VMEM) for x in arrays)


def row_of(index):
    return pl.ds(index * PROBES, PROBES)


def mirrored():
    core = lax.axis_index(CORE)
    pair = lax.axis_index(PAIR)

    def position(plane, row):
        return (plane + core * (1 - 2 * plane)) * ROWS + row + pair * (ROWS - 1 - 2 * row)

    return position


def prepare_kernel(
    signs_hbm, diag_hbm, own_ref, far_ref, high_ref, low_ref, signs_ref, diag_ref, arrived
):
    rows = 8 * CELLS
    copies = []
    for group in range(PROBES // 8):
        part = pl.ds(group * rows, rows)
        copies.append(pltpu.make_async_copy(signs_hbm.at[part, :], signs_ref.at[part, :], arrived.at[group]))
    lines = pltpu.make_async_copy(diag_hbm, diag_ref, arrived.at[PROBES // 8])
    lines.start()
    for copy in copies:
        copy.start()
    position = mirrored()

    lines.wait()
    for cell in range(CELLS):
        plane, row = divmod(cell, ROWS)
        line = diag_ref[pl.ds(position(plane, row), 1), :]
        own_ref[CELLS * PROBES + cell : CELLS * PROBES + cell + 1, :] = line
        for ref, step in ((low_ref, row), (high_ref, ROWS - 1 - row)):
            if step < 2:
                start = 6 * PROBES + plane * 2 + step
                ref[start : start + 1, :] = line
    for ref in (low_ref, high_ref):
        ref[6 * PROBES + 4 :, :] = jnp.zeros((4, LANES), F32)
    for group in range(PROBES // 8):
        copies[group].wait()
        for cell in range(CELLS):
            plane, row = divmod(cell, ROWS)
            bits = signs_ref[pl.ds(group * rows + position(plane, row), 8, stride=CELLS), :]
            probes = (2 * bits - 1).astype(F32)

            def put(ref, index):
                ref[pl.ds(index * PROBES + group * 8, 8), :] = probes

            put(own_ref, cell)
            if plane == 1:
                put(far_ref, row)
            for ref, step in ((low_ref, row), (high_ref, ROWS - 1 - row)):
                if step < 3:
                    put(ref, plane * 3 + step)


def prepare(signs, diagonal):
    hbm = pl.BlockSpec(memory_space=pltpu.HBM)
    return pl.pallas_call(
        prepare_kernel,
        out_shape=(
            shaped(OWN_ROWS, LANES),
            shaped(ROWS * PROBES, LANES),
            shaped(EDGE_ROWS, LANES),
            shaped(EDGE_ROWS, LANES),
        ),
        in_specs=[hbm, hbm],
        out_specs=tuple(vmem_specs(4)),
        scratch_shapes=[
            pltpu.VMEM((PROBES * CELLS, LANES), jnp.int32),
            pltpu.VMEM((CELLS, LANES), F32),
            pltpu.SemaphoreType.DMA((PROBES // 8 + 1,)),
        ],
        compiler_params=pltpu.CompilerParams(vmem_limit_bytes=VMEM_LIMIT),
        interpret=INTERPRET,
        name="prepare",
    )(*(pltpu.with_memory_space_constraint(x, pltpu.HBM) for x in (signs, diagonal)))


def pack_kernel(high_ref, low_ref, near_ref, corner_ref, cross_ref):
    def edge(plane, row):
        if row < 0:
            return low_ref[row_of(plane * 3 - row - 1), :]
        return high_ref[row_of(plane * 3 + row - ROWS), :]

    def edge_line(plane, row):
        ref = low_ref if row < 0 else high_ref
        start = 6 * PROBES + plane * 2
        return ref[start : start + 1, :]

    for row in range(ROWS):
        cross_ref[row_of(row), :] = near_ref[row_of(row), :]
    for ref, plane, first in ((corner_ref, 0, 0), (cross_ref, 1, ROWS)):
        for place, row in enumerate((-2, -1, ROWS, ROWS + 1)):
            ref[row_of(first + place), :] = edge(plane, row)
        for place, row in enumerate((-1, ROWS)):
            ref[row_of(first + 4 + place), :] = edge(1 - plane, row)
            start = (first + 6) * PROBES + place
            ref[start : start + 1, :] = edge_line(plane, row)
        ref[(first + 6) * PROBES + 2 :, :] = jnp.zeros((6, LANES), F32)


def pack(high, low, near):
    return pl.pallas_call(
        pack_kernel,
        out_shape=(shaped(CORNER_ROWS, LANES), shaped(CROSS_ROWS, LANES)),
        in_specs=vmem_specs(3),
        out_specs=tuple(vmem_specs(2)),
        compiler_params=pltpu.CompilerParams(vmem_limit_bytes=VMEM_LIMIT),
        interpret=INTERPRET,
        name="pack",
    )(*held(high, low, near))


def nt_dot(left, right):
    return lax.dot_general(left, right, (((1,), (1,)), ((), ())), preferred_element_type=F32)


def moved(value, blocks):
    return pltpu.roll(value, (blocks * PROBES) % LANES, 1)


def places():
    row = lax.broadcasted_iota(jnp.int32, (PROBES, LANES), 0)
    lane = lax.broadcasted_iota(jnp.int32, (PROBES, LANES), 1)
    return row, lane, lane % PROBES


def packed(first, last):
    row, lane, column = places()
    other = moved(last, -1)
    diagonals = jnp.sum(jnp.where(row == column, other, 0.0), axis=0, keepdims=True)
    slanted = pltpu.roll(jnp.broadcast_to(diagonals, (8, LANES)), 0, 1, stride=16, stride_axis=0)
    slanted = jnp.concatenate([slanted] * (PROBES // 8), 0)
    held_here = (row >= 17) & (row < 23) & (lane >= 96) & (lane < 112)
    return jnp.where(row <= column, first, jnp.where(held_here, slanted, other))


def unpacked(value):
    row, lane, column = places()
    turned = value.T
    turned = jnp.concatenate([turned[block * PROBES : (block + 1) * PROBES, :] for block in range(4)], 1)
    slanted = jnp.zeros((8, LANES), F32)
    for step in range(1, 7):
        mine = (row[:8] == step) & (lane[:8] // 16 == 6 - step)
        slanted = jnp.where(mine, pltpu.roll(value[16:24, :], LANES - 16 * step, 1), slanted)
    diagonals = jnp.sum(slanted, axis=0, keepdims=True)
    first = jnp.where(row <= column, value, turned)
    other = jnp.where(row == column, diagonals, jnp.where(row > column, value, turned))
    return first, moved(other, 1)


def basis_kernel(
    own_ref, high_ref, low_ref, near_ref, beside_ref, far_ref, corner_ref, cross_ref,
    split_out, gram_ref, first_ref, second_ref,
):
    def distance(plane):
        return -plane if plane < 0 else max(plane - (PLANES - 1), 0)

    def k0(plane, row):
        away = distance(plane)
        if away == 0:
            if row < 0:
                return low_ref[row_of(plane * 3 - row - 1), :]
            if row >= ROWS:
                return high_ref[row_of(plane * 3 + row - ROWS), :]
            return own_ref[row_of(plane * ROWS + row), :]
        if away == 3:
            return (far_ref if plane < 0 else cross_ref)[row_of(row), :]
        if 0 <= row < ROWS:
            if plane < 0:
                return near_ref[row_of((away - 1) * ROWS + row), :]
            return beside_ref[row_of((2 - away) * ROWS + row), :]
        ref, first = (corner_ref, 0) if plane < 0 else (cross_ref, ROWS)
        places = (-2, -1, ROWS, ROWS + 1) if away == 1 else (-1, ROWS)
        return ref[row_of(first + 4 * (away - 1) + places.index(row)), :]

    def factor(plane, row):
        away = distance(plane)
        if away == 0:
            if row < 0:
                ref, start = low_ref, 6 * PROBES + plane * 2 - row - 1
            elif row >= ROWS:
                ref, start = high_ref, 6 * PROBES + plane * 2 + row - ROWS
            else:
                ref, start = own_ref, CELLS * PROBES + plane * ROWS + row
        elif 0 <= row < ROWS:
            if plane < 0:
                ref, start = near_ref, CELLS * PROBES + (away - 1) * ROWS + row
            else:
                ref, start = beside_ref, CELLS * PROBES + (2 - away) * ROWS + row
        else:
            ref, first = (corner_ref, 0) if plane < 0 else (cross_ref, ROWS)
            start = (first + 6) * PROBES + (0 if row < 0 else 1)
        return ref[start : start + 1, :] + (6.0 - SHIFT)

    def cells(width):
        found = []
        for plane in range(-width, PLANES + width):
            extra = width - distance(plane)
            for row in range(-extra, ROWS + extra):
                found.append((plane, row))
        return found

    first_slot = {key: slot for slot, key in enumerate(cells(2))}
    second_slot = {key: slot for slot, key in enumerate(cells(1))}

    def k1(plane, row):
        return first_ref[row_of(first_slot[(plane, row)]), :]

    def k2(plane, row):
        return second_ref[row_of(second_slot[(plane, row)]), :]

    def apply(field, plane, row):
        center = field(plane, row)
        beside = field(plane - 1, row) + field(plane + 1, row)
        beside = beside + (field(plane, row - 1) + field(plane, row + 1))
        beside = beside + (pltpu.roll(center, 1, 1) + pltpu.roll(center, LANES - 1, 1))
        return factor(plane, row) * center - beside

    def keep(order, plane, row, value):
        columns = pl.ds((plane * ROWS + row) * LANES, LANES)
        upper = value.astype(BF16)
        split_out[row_of(order), columns] = upper
        if order == 0:
            split_out[row_of(4), columns] = jnp.zeros_like(upper)
        else:
            split_out[row_of(order + 4), columns] = (value - upper.astype(F32)).astype(BF16)

    for plane, row in cells(0):
        keep(0, plane, row, k0(plane, row))
    for plane, row in cells(2):
        value = apply(k0, plane, row)
        first_ref[row_of(first_slot[(plane, row)]), :] = value
        if distance(plane) == 0 and 0 <= row < ROWS:
            keep(1, plane, row, value)
    for plane, row in cells(1):
        value = apply(k1, plane, row) - B0 * k0(plane, row)
        second_ref[row_of(second_slot[(plane, row)]), :] = value
        if distance(plane) == 0 and 0 <= row < ROWS:
            keep(2, plane, row, value)
    for plane, row in cells(0):
        keep(3, plane, row, apply(k2, plane, row) - B1 * k1(plane, row))
    split = split_out[...]
    left = jnp.concatenate([split[:PROBES], split[3 * PROBES : 4 * PROBES], split[7 * PROBES :]], 0)
    product = nt_dot(left, split)
    product = product[:, :LANES] + product[:, LANES:]
    gram_ref[...] = packed(product[:PROBES], product[PROBES : 2 * PROBES] + product[2 * PROBES :])


def basis(*operands):
    width = CELLS * LANES
    return pl.pallas_call(
        basis_kernel,
        out_shape=(shaped(8 * PROBES, width, dtype=BF16), shaped(PROBES, LANES)),
        in_specs=vmem_specs(len(operands)),
        out_specs=tuple(vmem_specs(2)),
        scratch_shapes=[pltpu.VMEM((108 * PROBES, LANES), F32), pltpu.VMEM((68 * PROBES, LANES), F32)],
        compiler_params=pltpu.CompilerParams(vmem_limit_bytes=VMEM_LIMIT),
        interpret=INTERPRET,
        name="basis",
    )(*held(*operands))


def eliminate(system, block):
    groups = PROBES // 8
    lane = lax.broadcasted_iota(jnp.int32, (8, LANES), 1)
    sub = lax.broadcasted_iota(jnp.int32, (8, LANES), 0)
    start = block * PROBES
    inside = (lane >= start) & (lane < start + PROBES)
    pivoted = [system[8 * g : 8 * g + 8, :] for g in range(groups)]
    solved = [
        jnp.where(inside, jnp.where(lane - start == sub + 8 * g, 1.0, 0.0), pivoted[g]) for g in range(groups)
    ]
    scales = [None] * PROBES
    spread = {}

    def spread_panel(panel):
        for k in range(panel, min(panel + PANEL, PROBES)):
            for g in range(max(panel - PANEL, 0) // 8, groups):
                column = pivoted[g][:, start + k : start + k + 1]
                spread[k, g] = jnp.broadcast_to(column, (8, LANES))

    spread_panel(0)
    for panel in range(0, PROBES, PANEL):
        spread_panel(panel + PANEL)
        for k in range(panel, panel + PANEL):
            group, line = divmod(k, 8)

            def pivot_row(value):
                return jnp.broadcast_to(value[line : line + 1, :], (8, LANES))

            pivot = pivot_row(spread[k, group])
            inverse = 1.0 / pivot
            scales[k] = lax.rsqrt(pivot)
            multiplier = {}
            for g in range(group, groups):
                value = spread[k, g] * inverse
                if g == group:
                    value = jnp.where(sub > line, value, 0.0)
                multiplier[g] = value
            row = pivot_row(pivoted[group])
            solved_row = pivot_row(solved[group])
            for other in range(k + 1, min(panel + 2 * PANEL, PROBES)):
                weight = pivot_row(spread[other, group])
                for g in range(group, groups):
                    spread[other, g] = spread[other, g] - multiplier[g] * weight
            for g in range(group, groups):
                pivoted[g] = pivoted[g] - multiplier[g] * row
                solved[g] = solved[g] - multiplier[g] * solved_row
    upper = []
    for g in range(groups):
        scale = scales[8 * g]
        for line in range(1, 8):
            scale = jnp.where(sub == line, scales[8 * g + line], scale)
        solved[g] = solved[g] * scale
        upper.append(jnp.where(inside & (lane - start >= sub + 8 * g), pivoted[g] * scale, 0.0))
    return jnp.concatenate(solved, 0), jnp.concatenate(upper, 0)


def parts_of(value):
    upper = value.astype(BF16)
    rest = value - upper.astype(F32)
    middle = rest.astype(BF16)
    return upper, middle, (rest - middle.astype(F32)).astype(BF16)


def square(value):
    upper, middle, lower = parts_of(value)
    left = jnp.concatenate([upper, upper, middle, middle, upper, lower], 0)
    right = jnp.concatenate([upper, middle, upper, middle, lower, upper], 0)
    return lax.dot_general(left, right, (((0,), (0,)), ((), ())), preferred_element_type=F32)


def wide_dot(left, right):
    left_upper, left_lower, _ = parts_of(left)
    right_upper, right_lower, _ = parts_of(right)
    both = jnp.concatenate([left_upper, left_lower], 1)
    result = nt_dot(both, jnp.concatenate([right_upper, right_upper], 1))
    return result + nt_dot(both, jnp.concatenate([right_lower, right_lower], 1))


def finish_kernel(
    gram_ref, split_ref, alpha_hbm, beta_hbm, next_hbm, next_ref, alpha_ref, beta_ref, left, sent
):
    lane = lax.broadcasted_iota(jnp.int32, (PROBES, LANES), 1)
    block_of = lane // PROBES
    first, last = unpacked(gram_ref[...])
    second = moved(first, -1) + jnp.where(block_of == 1, B0, B1) * moved(first, 1)
    second = jnp.where(block_of == 3, moved(last, 2), jnp.where(block_of == 0, 0.0, second))
    third = moved(last, 1) + jnp.where(block_of == 2, B1 * moved(second, 1) - B0 * first, 0.0)
    third = jnp.where(block_of < 2, 0.0, third)
    systems = [first, second, third, jnp.where(block_of < 3, 0.0, last)]
    row32 = lax.broadcasted_iota(jnp.int32, (PROBES, PROBES), 0)
    lane32 = lax.broadcasted_iota(jnp.int32, (PROBES, PROBES), 1)
    solved = []
    beta = None
    for block in range(4):
        value, triangle = eliminate(systems[block], block)
        solved.append(value)
        if block < 3:
            update = square(value)
            for later in range(block + 1, 4):
                change = update[later * PROBES : (later + 1) * PROBES, :]
                change = jnp.where((block_of <= block) | (block_of >= later), change, 0.0)
                systems[later] = systems[later] - change
        if block > 0:
            beta = wide_dot(moved(triangle, -1), inverse)
            beta_ref[block - 1] = jnp.where(row32 <= lane32, beta, 0.0)
        if block < 3:
            inverse = jnp.where(block_of == block, value, 0.0)
            alpha = wide_dot(moved(value, -1), inverse)
            if block > 0:
                coupled = wide_dot(solved[block - 1], inverse)
                alpha = alpha - jnp.dot(
                    beta, coupled, precision=lax.Precision.HIGHEST, preferred_element_type=F32
                )
            alpha_ref[block] = alpha + jnp.where(row32 == lane32, SHIFT, 0.0)
    upper, lower, _ = parts_of(solved[3])
    weights = jnp.concatenate(
        [jnp.concatenate([upper, upper], 1), jnp.concatenate([lower, jnp.zeros_like(lower)], 1)], 0
    )
    position = mirrored()
    view = next_ref.reshape(PROBES, CELLS, LANES)
    copies = [
        pltpu.make_async_copy(alpha_ref, alpha_hbm, sent.at[0]),
        pltpu.make_async_copy(beta_ref, beta_hbm, sent.at[1]),
    ]
    for copy in copies:
        copy.start()
    for group in range(CELLS // 8):
        columns = pl.ds(group * 8 * LANES, 8 * LANES)
        result = jnp.dot(weights, split_ref[:, columns], preferred_element_type=F32)
        result = result[:PROBES] + result[PROBES:]
        for place in range(8):
            plane, row = divmod(group * 8 + place, ROWS)
            target = pl.ds(position(plane, row), PROBES, stride=CELLS)
            next_ref[target, :] = result[:, place * LANES : (place + 1) * LANES]
        plane, half = divmod(group, 2)
        core, pair = lax.axis_index(CORE), lax.axis_index(PAIR)
        first = (plane + core * (1 - 2 * plane)) * ROWS + (half + pair * (1 - 2 * half)) * 8
        part = pl.ds(pl.multiple_of(first, 8), 8)
        copy = pltpu.make_async_copy(view.at[:, part, :], next_hbm.at[:, part, :], left.at[group])
        copy.start()
        copies.append(copy)
    for copy in copies:
        copy.wait()


def finish(gram, split):
    return pl.pallas_call(
        finish_kernel,
        out_shape=(
            jax.ShapeDtypeStruct((3, PROBES, PROBES), F32),
            jax.ShapeDtypeStruct((3, PROBES, PROBES), F32),
            jax.ShapeDtypeStruct((PROBES, CELLS, LANES), F32),
        ),
        in_specs=vmem_specs(2),
        out_specs=(pl.BlockSpec(memory_space=pltpu.HBM),) * 3,
        scratch_shapes=[
            pltpu.VMEM((PROBES * CELLS, LANES), F32),
            pltpu.VMEM((3, PROBES, PROBES), F32),
            pltpu.VMEM((3, PROBES, PROBES), F32),
            pltpu.SemaphoreType.DMA((CELLS // 8,)),
            pltpu.SemaphoreType.DMA((2,)),
        ],
        compiler_params=pltpu.CompilerParams(vmem_limit_bytes=VMEM_LIMIT),
        interpret=INTERPRET,
        name="finish",
    )(*held(gram, split))


def off_chip(x):
    count = lax.axis_size(GX)
    return lax.ppermute(x, GX, [(i, (i - 1 if i % 2 == 0 else i + 1) % count) for i in range(count)])


def same_core(x):
    count = lax.axis_size(GX)
    return lax.ppermute(x, GX, [(i, (i + 2 if i % 2 == 0 else i - 2) % count) for i in range(count)])


def on_chip(x):
    count = lax.axis_size(CORE)
    return lax.ppermute(x, CORE, [(i, count - 1 - i) for i in range(count)])


def row_pair(x, offset):
    count = lax.axis_size(GY)
    step = lambda i: i + 1 if i % 2 == offset else i - 1
    return lax.ppermute(x, GY, [(i, step(i) % count) for i in range(count)])


def exchanged(x, axes):
    return lax.all_to_all(x, axes, 0, 0, tiled=True)


def gathered(x, axes):
    return exchanged(jnp.broadcast_to(x[None], (lax.axis_size(axes),) + x.shape), axes)


def reduced(x):
    near = lax.axis_size(NEAR)
    part = exchanged(x.reshape(near, x.shape[0] // near, x.shape[1]), NEAR).sum(0)
    part = gathered(part, FAR).sum(0)
    return gathered(part, NEAR).reshape(x.shape)


def per_device(probe_signs, diagonal):
    signs = probe_signs.reshape(PROBES * CELLS, LANES)
    diag = diagonal.reshape(CELLS, LANES)
    own, outer, top, bottom = prepare(signs, diag)
    near = off_chip(own)
    high = row_pair(top, 0)
    low = row_pair(bottom, 1)
    far = same_core(outer)
    beside = on_chip(own)
    corner_message, cross_message = pack(high, low, near)
    corner = off_chip(corner_message)
    cross = on_chip(cross_message)
    split, gram = basis(own, high, low, near, beside, far, corner, cross)
    alphas, betas, following = finish(reduced(gram), split)
    return (alphas, betas, following.reshape(PROBES, PLANES, ROWS, LANES))


def solution(mesh):
    split = Mesh(mesh.devices.reshape(2, 8, 2, 8, 2), ("gx_0", "gx_1", "gx_2", "gy_0", "gy_1"))
    placed = (P(None, GX, GY, None), P(GX, GY, None))
    return jax.shard_map(
        per_device,
        mesh=split,
        in_specs=placed,
        out_specs=(P(), P(), P(None, GX, GY, None)),
        check_vma=False,
    )
```

```python
import functools

import jax
import jax.numpy as jnp
from jax import lax
from jax.experimental import pallas as pl
from jax.experimental.pallas import tpu as pltpu
from jax.sharding import Mesh
from jax.sharding import PartitionSpec as P


GX = ("gx_0", "gx_1", "gx_2")
GY = ("gy_0", "gy_1")
NEAR = ("gx_0", "gx_2", "gy_1")
FAR = ("gx_1", "gy_0")
CORE = "gx_2"
PAIR = "gy_1"

PROBES = 32
LANES = 128
ROWS = 16
PLANES = 2
CELLS = PLANES * ROWS
SHIFT = 7.75
B0 = 7.0
B1 = 10.0
PANEL = 8
F32 = jnp.float32
BF16 = jnp.bfloat16
INTERPRET = False
VMEM_LIMIT = 16 * 2**20

OWN_ROWS = CELLS * PROBES + CELLS
EDGE_ROWS = 2 * 3 * PROBES + 8
MESSAGE_ROWS = (ROWS + 6) * PROBES + 8


def vmem_specs(count):
    return [pl.BlockSpec(memory_space=pltpu.VMEM) for _ in range(count)]


def shaped(*shape, dtype=F32):
    return pltpu.VMEM(shape, dtype)


def held(*arrays):
    return tuple(pltpu.with_memory_space_constraint(x, pltpu.VMEM) for x in arrays)


def row_of(index):
    return pl.ds(index * PROBES, PROBES)


def mirrored():
    core = lax.axis_index(CORE)
    pair = lax.axis_index(PAIR)

    def position(plane, row):
        return (plane + core * (1 - 2 * plane)) * ROWS + row + pair * (ROWS - 1 - 2 * row)

    return position


def prepare_kernel(
    signs_hbm, diag_hbm, own_ref, high_ref, low_ref, signs_ref, diag_ref, arrived
):
    rows = 8 * CELLS
    copies = []
    for group in range(PROBES // 8):
        part = pl.ds(group * rows, rows)
        copies.append(pltpu.make_async_copy(signs_hbm.at[part, :], signs_ref.at[part, :], arrived.at[group]))
    lines = pltpu.make_async_copy(diag_hbm, diag_ref, arrived.at[PROBES // 8])
    lines.start()
    for copy in copies:
        copy.start()
    position = mirrored()

    lines.wait()
    for cell in range(CELLS):
        plane, row = divmod(cell, ROWS)
        line = diag_ref[pl.ds(position(plane, row), 1), :]
        own_ref[CELLS * PROBES + cell : CELLS * PROBES + cell + 1, :] = line
        for ref, step in ((low_ref, row), (high_ref, ROWS - 1 - row)):
            if step < 2:
                start = 6 * PROBES + plane * 2 + step
                ref[start : start + 1, :] = line
    for ref in (low_ref, high_ref):
        ref[6 * PROBES + 4 :, :] = jnp.zeros((4, LANES), F32)
    for group in range(PROBES // 8):
        copies[group].wait()
        for cell in range(CELLS):
            plane, row = divmod(cell, ROWS)
            bits = signs_ref[pl.ds(group * rows + position(plane, row), 8, stride=CELLS), :]
            probes = (2 * bits - 1).astype(F32)

            def put(ref, index):
                ref[pl.ds(index * PROBES + group * 8, 8), :] = probes

            put(own_ref, cell)
            for ref, step in ((low_ref, row), (high_ref, ROWS - 1 - row)):
                if step < 3:
                    put(ref, plane * 3 + step)


def prepare(signs, diagonal):
    hbm = pl.BlockSpec(memory_space=pltpu.HBM)
    return pl.pallas_call(
        prepare_kernel,
        out_shape=(
            shaped(OWN_ROWS, LANES),
            shaped(EDGE_ROWS, LANES),
            shaped(EDGE_ROWS, LANES),
        ),
        in_specs=[hbm, hbm],
        out_specs=tuple(vmem_specs(3)),
        scratch_shapes=[
            pltpu.VMEM((PROBES * CELLS, LANES), jnp.int32),
            pltpu.VMEM((CELLS, LANES), F32),
            pltpu.SemaphoreType.DMA((PROBES // 8 + 1,)),
        ],
        compiler_params=pltpu.CompilerParams(vmem_limit_bytes=VMEM_LIMIT),
        interpret=INTERPRET,
        name="prepare",
    )(*(pltpu.with_memory_space_constraint(x, pltpu.HBM) for x in (signs, diagonal)))


def pack_kernel(plane, first_row, high_ref, low_ref, across_ref, message_ref):
    def edge(plane, row):
        if row < 0:
            return low_ref[row_of(plane * 3 - row - 1), :]
        return high_ref[row_of(plane * 3 + row - ROWS), :]

    for row in range(ROWS):
        message_ref[row_of(row), :] = across_ref[row_of(first_row + row), :]
    for place, row in enumerate((-2, -1, ROWS, ROWS + 1)):
        message_ref[row_of(ROWS + place), :] = edge(plane, row)
    for place, row in enumerate((-1, ROWS)):
        message_ref[row_of(ROWS + 4 + place), :] = edge(1 - plane, row)
        start = (ROWS + 6) * PROBES + place
        source = low_ref if row < 0 else high_ref
        line = 6 * PROBES + plane * 2
        message_ref[start : start + 1, :] = source[line : line + 1, :]
    message_ref[(ROWS + 6) * PROBES + 2 :, :] = jnp.zeros((6, LANES), F32)


def pack(plane, first_row, *operands):
    return pl.pallas_call(
        functools.partial(pack_kernel, plane, first_row),
        out_shape=shaped(MESSAGE_ROWS, LANES),
        in_specs=vmem_specs(len(operands)),
        out_specs=vmem_specs(1)[0],
        compiler_params=pltpu.CompilerParams(vmem_limit_bytes=VMEM_LIMIT),
        interpret=INTERPRET,
    )(*held(*operands))


def nt_dot(left, right):
    return lax.dot_general(left, right, (((1,), (1,)), ((), ())), preferred_element_type=F32)


def moved(value, blocks):
    return pltpu.roll(value, (blocks * PROBES) % LANES, 1)


def places():
    row = lax.broadcasted_iota(jnp.int32, (PROBES, LANES), 0)
    lane = lax.broadcasted_iota(jnp.int32, (PROBES, LANES), 1)
    return row, lane, lane % PROBES


def packed(first, last):
    row, lane, column = places()
    other = moved(last, -1)
    diagonals = jnp.sum(jnp.where(row == column, other, 0.0), axis=0, keepdims=True)
    slanted = pltpu.roll(jnp.broadcast_to(diagonals, (8, LANES)), 0, 1, stride=16, stride_axis=0)
    slanted = jnp.concatenate([slanted] * (PROBES // 8), 0)
    held_here = (row >= 17) & (row < 23) & (lane >= 96) & (lane < 112)
    return jnp.where(row <= column, first, jnp.where(held_here, slanted, other))


def unpacked(value):
    row, lane, column = places()
    turned = value.T
    turned = jnp.concatenate([turned[block * PROBES : (block + 1) * PROBES, :] for block in range(4)], 1)
    slanted = jnp.zeros((8, LANES), F32)
    for step in range(1, 7):
        mine = (row[:8] == step) & (lane[:8] // 16 == 6 - step)
        slanted = jnp.where(mine, pltpu.roll(value[16:24, :], LANES - 16 * step, 1), slanted)
    diagonals = jnp.sum(slanted, axis=0, keepdims=True)
    first = jnp.where(row <= column, value, turned)
    other = jnp.where(row == column, diagonals, jnp.where(row > column, value, turned))
    return first, moved(other, 1)


def basis_kernel(
    own_ref, high_ref, low_ref, near_ref, beside_ref, corner_ref, cross_ref,
    split_out, gram_ref, first_ref, second_ref,
):
    def distance(plane):
        return -plane if plane < 0 else max(plane - (PLANES - 1), 0)

    def k0(plane, row):
        away = distance(plane)
        if away == 0:
            if row < 0:
                return low_ref[row_of(plane * 3 - row - 1), :]
            if row >= ROWS:
                return high_ref[row_of(plane * 3 + row - ROWS), :]
            return own_ref[row_of(plane * ROWS + row), :]
        if away == 3:
            return (corner_ref if plane < 0 else cross_ref)[row_of(row), :]
        if 0 <= row < ROWS:
            if plane < 0:
                return near_ref[row_of((away - 1) * ROWS + row), :]
            return beside_ref[row_of((2 - away) * ROWS + row), :]
        ref = corner_ref if plane < 0 else cross_ref
        places = (-2, -1, ROWS, ROWS + 1) if away == 1 else (-1, ROWS)
        return ref[row_of(ROWS + 4 * (away - 1) + places.index(row)), :]

    def factor(plane, row):
        away = distance(plane)
        if away == 0:
            if row < 0:
                ref, start = low_ref, 6 * PROBES + plane * 2 - row - 1
            elif row >= ROWS:
                ref, start = high_ref, 6 * PROBES + plane * 2 + row - ROWS
            else:
                ref, start = own_ref, CELLS * PROBES + plane * ROWS + row
        elif 0 <= row < ROWS:
            if plane < 0:
                ref, start = near_ref, CELLS * PROBES + (away - 1) * ROWS + row
            else:
                ref, start = beside_ref, CELLS * PROBES + (2 - away) * ROWS + row
        else:
            ref = corner_ref if plane < 0 else cross_ref
            start = (ROWS + 6) * PROBES + (0 if row < 0 else 1)
        return ref[start : start + 1, :] + (6.0 - SHIFT)

    def cells(width):
        found = []
        for plane in range(-width, PLANES + width):
            extra = width - distance(plane)
            for row in range(-extra, ROWS + extra):
                found.append((plane, row))
        return found

    first_slot = {key: slot for slot, key in enumerate(cells(2))}
    second_slot = {key: slot for slot, key in enumerate(cells(1))}

    def k1(plane, row):
        return first_ref[row_of(first_slot[(plane, row)]), :]

    def k2(plane, row):
        return second_ref[row_of(second_slot[(plane, row)]), :]

    def apply(field, plane, row):
        center = field(plane, row)
        beside = field(plane - 1, row) + field(plane + 1, row)
        beside = beside + (field(plane, row - 1) + field(plane, row + 1))
        beside = beside + (pltpu.roll(center, 1, 1) + pltpu.roll(center, LANES - 1, 1))
        return factor(plane, row) * center - beside

    def keep(order, plane, row, value):
        columns = pl.ds((plane * ROWS + row) * LANES, LANES)
        upper = value.astype(BF16)
        split_out[row_of(order), columns] = upper
        if order == 0:
            split_out[row_of(4), columns] = jnp.zeros_like(upper)
        else:
            split_out[row_of(order + 4), columns] = (value - upper.astype(F32)).astype(BF16)

    for plane, row in cells(0):
        keep(0, plane, row, k0(plane, row))
    for plane, row in cells(2):
        value = apply(k0, plane, row)
        first_ref[row_of(first_slot[(plane, row)]), :] = value
        if distance(plane) == 0 and 0 <= row < ROWS:
            keep(1, plane, row, value)
    for plane, row in cells(1):
        value = apply(k1, plane, row) - B0 * k0(plane, row)
        second_ref[row_of(second_slot[(plane, row)]), :] = value
        if distance(plane) == 0 and 0 <= row < ROWS:
            keep(2, plane, row, value)
    for plane, row in cells(0):
        keep(3, plane, row, apply(k2, plane, row) - B1 * k1(plane, row))
    split = split_out[...]
    left = jnp.concatenate([split[:PROBES], split[3 * PROBES : 4 * PROBES], split[7 * PROBES :]], 0)
    product = nt_dot(left, split)
    product = product[:, :LANES] + product[:, LANES:]
    gram_ref[...] = packed(product[:PROBES], product[PROBES : 2 * PROBES] + product[2 * PROBES :])


def basis(*operands):
    width = CELLS * LANES
    return pl.pallas_call(
        basis_kernel,
        out_shape=(shaped(8 * PROBES, width, dtype=BF16), shaped(PROBES, LANES)),
        in_specs=vmem_specs(len(operands)),
        out_specs=tuple(vmem_specs(2)),
        scratch_shapes=[pltpu.VMEM((108 * PROBES, LANES), F32), pltpu.VMEM((68 * PROBES, LANES), F32)],
        compiler_params=pltpu.CompilerParams(vmem_limit_bytes=VMEM_LIMIT),
        interpret=INTERPRET,
        name="basis",
    )(*held(*operands))


def eliminate(system, block):
    groups = PROBES // 8
    lane = lax.broadcasted_iota(jnp.int32, (8, LANES), 1)
    sub = lax.broadcasted_iota(jnp.int32, (8, LANES), 0)
    start = block * PROBES
    inside = (lane >= start) & (lane < start + PROBES)
    pivoted = [system[8 * g : 8 * g + 8, :] for g in range(groups)]
    solved = [
        jnp.where(inside, jnp.where(lane - start == sub + 8 * g, 1.0, 0.0), pivoted[g]) for g in range(groups)
    ]
    scales = [None] * PROBES
    spread = {}

    def spread_panel(panel):
        for k in range(panel, min(panel + PANEL, PROBES)):
            for g in range(max(panel - PANEL, 0) // 8, groups):
                column = pivoted[g][:, start + k : start + k + 1]
                spread[k, g] = jnp.broadcast_to(column, (8, LANES))

    spread_panel(0)
    for panel in range(0, PROBES, PANEL):
        spread_panel(panel + PANEL)
        for k in range(panel, panel + PANEL):
            group, line = divmod(k, 8)

            def pivot_row(value):
                return jnp.broadcast_to(value[line : line + 1, :], (8, LANES))

            pivot = pivot_row(spread[k, group])
            inverse = 1.0 / pivot
            scales[k] = lax.rsqrt(pivot)
            multiplier = {}
            for g in range(group, groups):
                value = spread[k, g] * inverse
                if g == group:
                    value = jnp.where(sub > line, value, 0.0)
                multiplier[g] = value
            row = pivot_row(pivoted[group])
            solved_row = pivot_row(solved[group])
            for other in range(k + 1, min(panel + 2 * PANEL, PROBES)):
                weight = pivot_row(spread[other, group])
                for g in range(group, groups):
                    spread[other, g] = spread[other, g] - multiplier[g] * weight
            for g in range(group, groups):
                pivoted[g] = pivoted[g] - multiplier[g] * row
                solved[g] = solved[g] - multiplier[g] * solved_row
    upper = []
    for g in range(groups):
        scale = scales[8 * g]
        for line in range(1, 8):
            scale = jnp.where(sub == line, scales[8 * g + line], scale)
        solved[g] = solved[g] * scale
        upper.append(jnp.where(inside & (lane - start >= sub + 8 * g), pivoted[g] * scale, 0.0))
    return jnp.concatenate(solved, 0), jnp.concatenate(upper, 0)


def parts_of(value):
    upper = value.astype(BF16)
    rest = value - upper.astype(F32)
    middle = rest.astype(BF16)
    return upper, middle, (rest - middle.astype(F32)).astype(BF16)


def square(value):
    upper, middle, lower = parts_of(value)
    left = jnp.concatenate([upper, upper, middle, middle, upper, lower], 0)
    right = jnp.concatenate([upper, middle, upper, middle, lower, upper], 0)
    return lax.dot_general(left, right, (((0,), (0,)), ((), ())), preferred_element_type=F32)


def wide_dot(left, right):
    left_upper, left_lower, _ = parts_of(left)
    right_upper, right_lower, _ = parts_of(right)
    both = jnp.concatenate([left_upper, left_lower], 1)
    result = nt_dot(both, jnp.concatenate([right_upper, right_upper], 1))
    return result + nt_dot(both, jnp.concatenate([right_lower, right_lower], 1))


def finish_kernel(
    gram_ref, split_ref, alpha_hbm, beta_hbm, next_hbm, next_ref, alpha_ref, beta_ref, left, sent
):
    lane = lax.broadcasted_iota(jnp.int32, (PROBES, LANES), 1)
    block_of = lane // PROBES
    first, last = unpacked(gram_ref[...])
    second = moved(first, -1) + jnp.where(block_of == 1, B0, B1) * moved(first, 1)
    second = jnp.where(block_of == 3, moved(last, 2), jnp.where(block_of == 0, 0.0, second))
    third = moved(last, 1) + jnp.where(block_of == 2, B1 * moved(second, 1) - B0 * first, 0.0)
    third = jnp.where(block_of < 2, 0.0, third)
    systems = [first, second, third, jnp.where(block_of < 3, 0.0, last)]
    row32 = lax.broadcasted_iota(jnp.int32, (PROBES, PROBES), 0)
    lane32 = lax.broadcasted_iota(jnp.int32, (PROBES, PROBES), 1)
    solved = []
    beta = None
    for block in range(4):
        value, triangle = eliminate(systems[block], block)
        solved.append(value)
        if block < 3:
            update = square(value)
            for later in range(block + 1, 4):
                change = update[later * PROBES : (later + 1) * PROBES, :]
                change = jnp.where((block_of <= block) | (block_of >= later), change, 0.0)
                systems[later] = systems[later] - change
        if block > 0:
            beta = wide_dot(moved(triangle, -1), inverse)
            beta_ref[block - 1] = jnp.where(row32 <= lane32, beta, 0.0)
        if block < 3:
            inverse = jnp.where(block_of == block, value, 0.0)
            alpha = wide_dot(moved(value, -1), inverse)
            if block > 0:
                coupled = wide_dot(solved[block - 1], inverse)
                alpha = alpha - jnp.dot(
                    beta, coupled, precision=lax.Precision.HIGHEST, preferred_element_type=F32
                )
            alpha_ref[block] = alpha + jnp.where(row32 == lane32, SHIFT, 0.0)
    upper, lower, _ = parts_of(solved[3])
    weights = jnp.concatenate(
        [jnp.concatenate([upper, upper], 1), jnp.concatenate([lower, jnp.zeros_like(lower)], 1)], 0
    )
    position = mirrored()
    view = next_ref.reshape(PROBES, CELLS, LANES)
    copies = [
        pltpu.make_async_copy(alpha_ref, alpha_hbm, sent.at[0]),
        pltpu.make_async_copy(beta_ref, beta_hbm, sent.at[1]),
    ]
    for copy in copies:
        copy.start()
    for group in range(CELLS // 8):
        columns = pl.ds(group * 8 * LANES, 8 * LANES)
        result = jnp.dot(weights, split_ref[:, columns], preferred_element_type=F32)
        result = result[:PROBES] + result[PROBES:]
        for place in range(8):
            plane, row = divmod(group * 8 + place, ROWS)
            target = pl.ds(position(plane, row), PROBES, stride=CELLS)
            next_ref[target, :] = result[:, place * LANES : (place + 1) * LANES]
        plane, half = divmod(group, 2)
        core, pair = lax.axis_index(CORE), lax.axis_index(PAIR)
        first = (plane + core * (1 - 2 * plane)) * ROWS + (half + pair * (1 - 2 * half)) * 8
        part = pl.ds(pl.multiple_of(first, 8), 8)
        copy = pltpu.make_async_copy(view.at[:, part, :], next_hbm.at[:, part, :], left.at[group])
        copy.start()
        copies.append(copy)
    for copy in copies:
        copy.wait()


def finish(gram, split):
    return pl.pallas_call(
        finish_kernel,
        out_shape=(
            jax.ShapeDtypeStruct((3, PROBES, PROBES), F32),
            jax.ShapeDtypeStruct((3, PROBES, PROBES), F32),
            jax.ShapeDtypeStruct((PROBES, CELLS, LANES), F32),
        ),
        in_specs=vmem_specs(2),
        out_specs=(pl.BlockSpec(memory_space=pltpu.HBM),) * 3,
        scratch_shapes=[
            pltpu.VMEM((PROBES * CELLS, LANES), F32),
            pltpu.VMEM((3, PROBES, PROBES), F32),
            pltpu.VMEM((3, PROBES, PROBES), F32),
            pltpu.SemaphoreType.DMA((CELLS // 8,)),
            pltpu.SemaphoreType.DMA((2,)),
        ],
        compiler_params=pltpu.CompilerParams(vmem_limit_bytes=VMEM_LIMIT),
        interpret=INTERPRET,
        name="finish",
    )(*held(gram, split))


def off_chip(x):
    count = lax.axis_size(GX)
    return lax.ppermute(x, GX, [(i, (i - 1 if i % 2 == 0 else i + 1) % count) for i in range(count)])


def on_chip(x):
    count = lax.axis_size(CORE)
    return lax.ppermute(x, CORE, [(i, count - 1 - i) for i in range(count)])


def row_pair(x, offset):
    count = lax.axis_size(GY)
    step = lambda i: i + 1 if i % 2 == offset else i - 1
    return lax.ppermute(x, GY, [(i, step(i) % count) for i in range(count)])


def exchanged(x, axes):
    return lax.all_to_all(x, axes, 0, 0, tiled=True)


def gathered(x, axes):
    return exchanged(jnp.broadcast_to(x[None], (lax.axis_size(axes),) + x.shape), axes)


def reduced(x):
    near = lax.axis_size(NEAR)
    part = exchanged(x.reshape(near, x.shape[0] // near, x.shape[1]), NEAR).sum(0)
    part = gathered(part, FAR).sum(0)
    return gathered(part, NEAR).reshape(x.shape)


def per_device(probe_signs, diagonal):
    signs = probe_signs.reshape(PROBES * CELLS, LANES)
    diag = diagonal.reshape(CELLS, LANES)
    own, top, bottom = prepare(signs, diag)
    high = row_pair(top, 0)
    low = row_pair(bottom, 1)
    near = off_chip(own)
    beside = on_chip(own)
    corner_message = pack(0, ROWS, high, low, beside)
    corner = off_chip(corner_message)
    cross_message = pack(1, 0, high, low, near)
    cross = on_chip(cross_message)
    split, gram = basis(own, high, low, near, beside, corner, cross)
    alphas, betas, following = finish(reduced(gram), split)
    return (alphas, betas, following.reshape(PROBES, PLANES, ROWS, LANES))


def solution(mesh):
    split = Mesh(mesh.devices.reshape(2, 8, 2, 8, 2), ("gx_0", "gx_1", "gx_2", "gy_0", "gy_1"))
    placed = (P(None, GX, GY, None), P(GX, GY, None))
    return jax.shard_map(
        per_device,
        mesh=split,
        in_specs=placed,
        out_specs=(P(), P(), P(None, GX, GY, None)),
        check_vma=False,
    )
```

```python
import functools

import jax
import jax.numpy as jnp
from jax import lax
from jax.experimental import pallas as pl
from jax.experimental.pallas import tpu as pltpu
from jax.sharding import Mesh
from jax.sharding import PartitionSpec as P


GX = ("gx_0", "gx_1", "gx_2")
GY = ("gy_0", "gy_1")
NEAR = ("gx_0", "gx_2", "gy_1")
FAR = ("gx_1", "gy_0")
CORE = "gx_2"
PAIR = "gy_1"

PROBES = 32
LANES = 128
ROWS = 16
PLANES = 2
CELLS = PLANES * ROWS
SHIFT = 7.75
B0 = 7.0
B1 = 10.0
PANEL = 8
F32 = jnp.float32
BF16 = jnp.bfloat16
INTERPRET = False
VMEM_LIMIT = 16 * 2**20

OWN_ROWS = CELLS * PROBES + CELLS
EDGE_ROWS = 2 * 3 * PROBES + 8
MESSAGE_ROWS = (ROWS + 6) * PROBES + 8


def vmem_specs(count):
    return [pl.BlockSpec(memory_space=pltpu.VMEM) for _ in range(count)]


def shaped(*shape, dtype=F32):
    return pltpu.VMEM(shape, dtype)


def held(*arrays):
    return tuple(pltpu.with_memory_space_constraint(x, pltpu.VMEM) for x in arrays)


def row_of(index):
    return pl.ds(index * PROBES, PROBES)


def mirrored():
    core = lax.axis_index(CORE)
    pair = lax.axis_index(PAIR)

    def position(plane, row):
        return (plane + core * (1 - 2 * plane)) * ROWS + row + pair * (ROWS - 1 - 2 * row)

    return position


def prepare_kernel(
    signs_hbm, diag_hbm, own_ref, high_ref, low_ref, signs_ref, diag_ref, arrived
):
    rows = 8 * CELLS
    copies = []
    for group in range(PROBES // 8):
        part = pl.ds(group * rows, rows)
        copies.append(pltpu.make_async_copy(signs_hbm.at[part, :], signs_ref.at[part, :], arrived.at[group]))
    lines = pltpu.make_async_copy(diag_hbm, diag_ref, arrived.at[PROBES // 8])
    lines.start()
    for copy in copies:
        copy.start()
    position = mirrored()

    lines.wait()
    for cell in range(CELLS):
        plane, row = divmod(cell, ROWS)
        line = diag_ref[pl.ds(position(plane, row), 1), :]
        own_ref[CELLS * PROBES + cell : CELLS * PROBES + cell + 1, :] = line
        for ref, step in ((low_ref, row), (high_ref, ROWS - 1 - row)):
            if step < 2:
                start = 6 * PROBES + plane * 2 + step
                ref[start : start + 1, :] = line
    for ref in (low_ref, high_ref):
        ref[6 * PROBES + 4 :, :] = jnp.zeros((4, LANES), F32)
    for group in range(PROBES // 8):
        copies[group].wait()
        for cell in range(CELLS):
            plane, row = divmod(cell, ROWS)
            bits = signs_ref[pl.ds(group * rows + position(plane, row), 8, stride=CELLS), :]
            probes = (2 * bits - 1).astype(F32)

            def put(ref, index):
                ref[pl.ds(index * PROBES + group * 8, 8), :] = probes

            put(own_ref, cell)
            for ref, step in ((low_ref, row), (high_ref, ROWS - 1 - row)):
                if step < 3:
                    put(ref, plane * 3 + step)


def prepare(signs, diagonal):
    hbm = pl.BlockSpec(memory_space=pltpu.HBM)
    return pl.pallas_call(
        prepare_kernel,
        out_shape=(
            shaped(OWN_ROWS, LANES),
            shaped(EDGE_ROWS, LANES),
            shaped(EDGE_ROWS, LANES),
        ),
        in_specs=[hbm, hbm],
        out_specs=tuple(vmem_specs(3)),
        scratch_shapes=[
            pltpu.VMEM((PROBES * CELLS, LANES), jnp.int32),
            pltpu.VMEM((CELLS, LANES), F32),
            pltpu.SemaphoreType.DMA((PROBES // 8 + 1,)),
        ],
        compiler_params=pltpu.CompilerParams(vmem_limit_bytes=VMEM_LIMIT),
        interpret=INTERPRET,
        name="prepare",
    )(*(pltpu.with_memory_space_constraint(x, pltpu.HBM) for x in (signs, diagonal)))


def pack_kernel(plane, first_row, high_ref, low_ref, across_ref, message_ref):
    def edge(plane, row):
        if row < 0:
            return low_ref[row_of(plane * 3 - row - 1), :]
        return high_ref[row_of(plane * 3 + row - ROWS), :]

    for row in range(ROWS):
        message_ref[row_of(row), :] = across_ref[row_of(first_row + row), :]
    for place, row in enumerate((-2, -1, ROWS, ROWS + 1)):
        message_ref[row_of(ROWS + place), :] = edge(plane, row)
    for place, row in enumerate((-1, ROWS)):
        message_ref[row_of(ROWS + 4 + place), :] = edge(1 - plane, row)
        start = (ROWS + 6) * PROBES + place
        source = low_ref if row < 0 else high_ref
        line = 6 * PROBES + plane * 2
        message_ref[start : start + 1, :] = source[line : line + 1, :]
    message_ref[(ROWS + 6) * PROBES + 2 :, :] = jnp.zeros((6, LANES), F32)


def pack(plane, first_row, *operands):
    return pl.pallas_call(
        functools.partial(pack_kernel, plane, first_row),
        out_shape=shaped(MESSAGE_ROWS, LANES),
        in_specs=vmem_specs(len(operands)),
        out_specs=vmem_specs(1)[0],
        compiler_params=pltpu.CompilerParams(vmem_limit_bytes=VMEM_LIMIT),
        interpret=INTERPRET,
    )(*held(*operands))


def nt_dot(left, right):
    return lax.dot_general(left, right, (((1,), (1,)), ((), ())), preferred_element_type=F32)


def moved(value, blocks):
    return pltpu.roll(value, (blocks * PROBES) % LANES, 1)


def places():
    row = lax.broadcasted_iota(jnp.int32, (PROBES, LANES), 0)
    lane = lax.broadcasted_iota(jnp.int32, (PROBES, LANES), 1)
    return row, lane, lane % PROBES


def packed(first, last):
    row, lane, column = places()
    other = moved(last, -1)
    diagonals = jnp.sum(jnp.where(row == column, other, 0.0), axis=0, keepdims=True)
    slanted = pltpu.roll(jnp.broadcast_to(diagonals, (8, LANES)), 0, 1, stride=16, stride_axis=0)
    slanted = jnp.concatenate([slanted] * (PROBES // 8), 0)
    held_here = (row >= 17) & (row < 23) & (lane >= 96) & (lane < 112)
    return jnp.where(row <= column, first, jnp.where(held_here, slanted, other))


def unpacked(value):
    row, lane, column = places()
    turned = value.T
    turned = jnp.concatenate([turned[block * PROBES : (block + 1) * PROBES, :] for block in range(4)], 1)
    slanted = jnp.zeros((8, LANES), F32)
    for step in range(1, 7):
        mine = (row[:8] == step) & (lane[:8] // 16 == 6 - step)
        slanted = jnp.where(mine, pltpu.roll(value[16:24, :], LANES - 16 * step, 1), slanted)
    diagonals = jnp.sum(slanted, axis=0, keepdims=True)
    first = jnp.where(row <= column, value, turned)
    other = jnp.where(row == column, diagonals, jnp.where(row > column, value, turned))
    return first, moved(other, 1)


def distance(plane):
    return -plane if plane < 0 else max(plane - (PLANES - 1), 0)


def cells(width):
    found = []
    for plane in range(-width, PLANES + width):
        extra = width - distance(plane)
        for row in range(-extra, ROWS + extra):
            found.append((plane, row))
    return found


def known_early(order, plane, row):
    if order == 0:
        return distance(plane) == 0 or (distance(plane) < 3 and 0 <= row < ROWS)
    around = [(plane, row), (plane - 1, row), (plane + 1, row), (plane, row - 1), (plane, row + 1)]
    return all(known_early(order - 1, *cell) for cell in around)


def slots(order, width, early):
    chosen = [cell for cell in cells(width) if known_early(order, *cell) == early]
    return {cell: slot for slot, cell in enumerate(chosen)}


FIRST_EARLY, FIRST_LATE = slots(1, 2, True), slots(1, 2, False)
SECOND_EARLY, SECOND_LATE = slots(2, 1, True), slots(2, 1, False)


class Fields:
    def __init__(self, own, high, low, near, beside, corner, cross, first, second, split):
        self.own, self.high, self.low, self.near, self.beside = own, high, low, near, beside
        self.corner, self.cross = corner, cross
        self.first, self.second, self.split = first, second, split

    def k0(self, plane, row):
        away = distance(plane)
        if away == 0:
            if row < 0:
                return self.low[row_of(plane * 3 - row - 1), :]
            if row >= ROWS:
                return self.high[row_of(plane * 3 + row - ROWS), :]
            return self.own[row_of(plane * ROWS + row), :]
        if away == 3:
            return (self.corner if plane < 0 else self.cross)[row_of(row), :]
        if 0 <= row < ROWS:
            if plane < 0:
                return self.near[row_of((away - 1) * ROWS + row), :]
            return self.beside[row_of((2 - away) * ROWS + row), :]
        ref = self.corner if plane < 0 else self.cross
        known = (-2, -1, ROWS, ROWS + 1) if away == 1 else (-1, ROWS)
        return ref[row_of(ROWS + 4 * (away - 1) + known.index(row)), :]

    def factor(self, plane, row):
        away = distance(plane)
        if away == 0:
            if row < 0:
                ref, start = self.low, 6 * PROBES + plane * 2 - row - 1
            elif row >= ROWS:
                ref, start = self.high, 6 * PROBES + plane * 2 + row - ROWS
            else:
                ref, start = self.own, CELLS * PROBES + plane * ROWS + row
        elif 0 <= row < ROWS:
            if plane < 0:
                ref, start = self.near, CELLS * PROBES + (away - 1) * ROWS + row
            else:
                ref, start = self.beside, CELLS * PROBES + (2 - away) * ROWS + row
        else:
            ref = self.corner if plane < 0 else self.cross
            start = (ROWS + 6) * PROBES + (0 if row < 0 else 1)
        return ref[start : start + 1, :] + (6.0 - SHIFT)

    def k1(self, plane, row):
        early = (plane, row) in FIRST_EARLY
        slot = (FIRST_EARLY if early else FIRST_LATE)[(plane, row)]
        return self.first[0 if early else 1][row_of(slot), :]

    def k2(self, plane, row):
        early = (plane, row) in SECOND_EARLY
        slot = (SECOND_EARLY if early else SECOND_LATE)[(plane, row)]
        return self.second[0 if early else 1][row_of(slot), :]

    def apply(self, field, plane, row):
        center = field(plane, row)
        beside = field(plane - 1, row) + field(plane + 1, row)
        beside = beside + (field(plane, row - 1) + field(plane, row + 1))
        beside = beside + (pltpu.roll(center, 1, 1) + pltpu.roll(center, LANES - 1, 1))
        return self.factor(plane, row) * center - beside

    def keep(self, order, plane, row, value):
        if distance(plane) > 0 or not 0 <= row < ROWS:
            return
        columns = pl.ds((plane * ROWS + row) * LANES, LANES)
        upper = value.astype(BF16)
        self.split[row_of(order), columns] = upper
        if order == 0:
            self.split[row_of(4), columns] = jnp.zeros_like(upper)
        else:
            self.split[row_of(order + 4), columns] = (value - upper.astype(F32)).astype(BF16)

    def fill(self, early):
        side = 0 if early else 1
        for (plane, row), slot in (FIRST_EARLY if early else FIRST_LATE).items():
            value = self.apply(self.k0, plane, row)
            self.first[side][row_of(slot), :] = value
            self.keep(1, plane, row, value)
        for (plane, row), slot in (SECOND_EARLY if early else SECOND_LATE).items():
            value = self.apply(self.k1, plane, row) - B0 * self.k0(plane, row)
            self.second[side][row_of(slot), :] = value
            self.keep(2, plane, row, value)


def early_kernel(own_ref, high_ref, low_ref, near_ref, beside_ref, split_ref, first_ref, second_ref):
    fields = Fields(
        own_ref, high_ref, low_ref, near_ref, beside_ref, None, None, (first_ref, None), (second_ref, None), split_ref
    )
    for plane, row in cells(0):
        fields.keep(0, plane, row, fields.k0(plane, row))
    fields.fill(True)


def late_kernel(
    own_ref, high_ref, low_ref, near_ref, beside_ref, corner_ref, cross_ref, first_ref, second_ref, split_in,
    split_ref, gram_ref, first_late, second_late,
):
    fields = Fields(
        own_ref, high_ref, low_ref, near_ref, beside_ref, corner_ref, cross_ref,
        (first_ref, first_late), (second_ref, second_late), split_ref,
    )
    fields.fill(False)
    for plane, row in cells(0):
        fields.keep(3, plane, row, fields.apply(fields.k2, plane, row) - B1 * fields.k1(plane, row))
    split = split_ref[...]
    left = jnp.concatenate([split[:PROBES], split[3 * PROBES : 4 * PROBES], split[7 * PROBES :]], 0)
    product = nt_dot(left, split)
    product = product[:, :LANES] + product[:, LANES:]
    gram_ref[...] = packed(product[:PROBES], product[PROBES : 2 * PROBES] + product[2 * PROBES :])


def basis_early(*operands):
    return pl.pallas_call(
        early_kernel,
        out_shape=(
            shaped(8 * PROBES, CELLS * LANES, dtype=BF16),
            shaped(len(FIRST_EARLY) * PROBES, LANES),
            shaped(len(SECOND_EARLY) * PROBES, LANES),
        ),
        in_specs=vmem_specs(len(operands)),
        out_specs=tuple(vmem_specs(3)),
        compiler_params=pltpu.CompilerParams(vmem_limit_bytes=VMEM_LIMIT),
        interpret=INTERPRET,
        name="basis_early",
    )(*held(*operands))


def basis_late(*operands):
    return pl.pallas_call(
        late_kernel,
        out_shape=(shaped(8 * PROBES, CELLS * LANES, dtype=BF16), shaped(PROBES, LANES)),
        in_specs=vmem_specs(len(operands)),
        out_specs=tuple(vmem_specs(2)),
        scratch_shapes=[
            pltpu.VMEM((len(FIRST_LATE) * PROBES, LANES), F32),
            pltpu.VMEM((len(SECOND_LATE) * PROBES, LANES), F32),
        ],
        input_output_aliases={len(operands) - 1: 0},
        compiler_params=pltpu.CompilerParams(vmem_limit_bytes=VMEM_LIMIT),
        interpret=INTERPRET,
        name="basis_late",
    )(*held(*operands))


def eliminate(system, block):
    groups = PROBES // 8
    lane = lax.broadcasted_iota(jnp.int32, (8, LANES), 1)
    sub = lax.broadcasted_iota(jnp.int32, (8, LANES), 0)
    start = block * PROBES
    inside = (lane >= start) & (lane < start + PROBES)
    pivoted = [system[8 * g : 8 * g + 8, :] for g in range(groups)]
    solved = [
        jnp.where(inside, jnp.where(lane - start == sub + 8 * g, 1.0, 0.0), pivoted[g]) for g in range(groups)
    ]
    scales = [None] * PROBES
    spread = {}

    def spread_panel(panel):
        for k in range(panel, min(panel + PANEL, PROBES)):
            for g in range(max(panel - PANEL, 0) // 8, groups):
                column = pivoted[g][:, start + k : start + k + 1]
                spread[k, g] = jnp.broadcast_to(column, (8, LANES))

    spread_panel(0)
    for panel in range(0, PROBES, PANEL):
        spread_panel(panel + PANEL)
        for k in range(panel, panel + PANEL):
            group, line = divmod(k, 8)

            def pivot_row(value):
                return jnp.broadcast_to(value[line : line + 1, :], (8, LANES))

            pivot = pivot_row(spread[k, group])
            inverse = 1.0 / pivot
            scales[k] = lax.rsqrt(pivot)
            multiplier = {}
            for g in range(group, groups):
                value = spread[k, g] * inverse
                if g == group:
                    value = jnp.where(sub > line, value, 0.0)
                multiplier[g] = value
            row = pivot_row(pivoted[group])
            solved_row = pivot_row(solved[group])
            for other in range(k + 1, min(panel + 2 * PANEL, PROBES)):
                weight = pivot_row(spread[other, group])
                for g in range(group, groups):
                    spread[other, g] = spread[other, g] - multiplier[g] * weight
            for g in range(group, groups):
                pivoted[g] = pivoted[g] - multiplier[g] * row
                solved[g] = solved[g] - multiplier[g] * solved_row
    upper = []
    for g in range(groups):
        scale = scales[8 * g]
        for line in range(1, 8):
            scale = jnp.where(sub == line, scales[8 * g + line], scale)
        solved[g] = solved[g] * scale
        upper.append(jnp.where(inside & (lane - start >= sub + 8 * g), pivoted[g] * scale, 0.0))
    return jnp.concatenate(solved, 0), jnp.concatenate(upper, 0)


def parts_of(value):
    upper = value.astype(BF16)
    rest = value - upper.astype(F32)
    middle = rest.astype(BF16)
    return upper, middle, (rest - middle.astype(F32)).astype(BF16)


def square(value):
    upper, middle, lower = parts_of(value)
    left = jnp.concatenate([upper, upper, middle, middle, upper, lower], 0)
    right = jnp.concatenate([upper, middle, upper, middle, lower, upper], 0)
    return lax.dot_general(left, right, (((0,), (0,)), ((), ())), preferred_element_type=F32)


def wide_dot(left, right):
    left_upper, left_lower, _ = parts_of(left)
    right_upper, right_lower, _ = parts_of(right)
    both = jnp.concatenate([left_upper, left_lower], 1)
    result = nt_dot(both, jnp.concatenate([right_upper, right_upper], 1))
    return result + nt_dot(both, jnp.concatenate([right_lower, right_lower], 1))


def finish_kernel(
    gram_ref, split_ref, alpha_hbm, beta_hbm, next_hbm, next_ref, alpha_ref, beta_ref, left, sent
):
    lane = lax.broadcasted_iota(jnp.int32, (PROBES, LANES), 1)
    block_of = lane // PROBES
    first, last = unpacked(gram_ref[...])
    second = moved(first, -1) + jnp.where(block_of == 1, B0, B1) * moved(first, 1)
    second = jnp.where(block_of == 3, moved(last, 2), jnp.where(block_of == 0, 0.0, second))
    third = moved(last, 1) + jnp.where(block_of == 2, B1 * moved(second, 1) - B0 * first, 0.0)
    third = jnp.where(block_of < 2, 0.0, third)
    systems = [first, second, third, jnp.where(block_of < 3, 0.0, last)]
    row32 = lax.broadcasted_iota(jnp.int32, (PROBES, PROBES), 0)
    lane32 = lax.broadcasted_iota(jnp.int32, (PROBES, PROBES), 1)
    solved = []
    beta = None
    for block in range(4):
        value, triangle = eliminate(systems[block], block)
        solved.append(value)
        if block < 3:
            update = square(value)
            for later in range(block + 1, 4):
                change = update[later * PROBES : (later + 1) * PROBES, :]
                change = jnp.where((block_of <= block) | (block_of >= later), change, 0.0)
                systems[later] = systems[later] - change
        if block > 0:
            beta = wide_dot(moved(triangle, -1), inverse)
            beta_ref[block - 1] = jnp.where(row32 <= lane32, beta, 0.0)
        if block < 3:
            inverse = jnp.where(block_of == block, value, 0.0)
            alpha = wide_dot(moved(value, -1), inverse)
            if block > 0:
                coupled = wide_dot(solved[block - 1], inverse)
                alpha = alpha - jnp.dot(
                    beta, coupled, precision=lax.Precision.HIGHEST, preferred_element_type=F32
                )
            alpha_ref[block] = alpha + jnp.where(row32 == lane32, SHIFT, 0.0)
    upper, lower, _ = parts_of(solved[3])
    weights = jnp.concatenate(
        [jnp.concatenate([upper, upper], 1), jnp.concatenate([lower, jnp.zeros_like(lower)], 1)], 0
    )
    position = mirrored()
    view = next_ref.reshape(PROBES, CELLS, LANES)
    copies = [
        pltpu.make_async_copy(alpha_ref, alpha_hbm, sent.at[0]),
        pltpu.make_async_copy(beta_ref, beta_hbm, sent.at[1]),
    ]
    for copy in copies:
        copy.start()
    for group in range(CELLS // 8):
        columns = pl.ds(group * 8 * LANES, 8 * LANES)
        result = jnp.dot(weights, split_ref[:, columns], preferred_element_type=F32)
        result = result[:PROBES] + result[PROBES:]
        for place in range(8):
            plane, row = divmod(group * 8 + place, ROWS)
            target = pl.ds(position(plane, row), PROBES, stride=CELLS)
            next_ref[target, :] = result[:, place * LANES : (place + 1) * LANES]
        plane, half = divmod(group, 2)
        core, pair = lax.axis_index(CORE), lax.axis_index(PAIR)
        first = (plane + core * (1 - 2 * plane)) * ROWS + (half + pair * (1 - 2 * half)) * 8
        part = pl.ds(pl.multiple_of(first, 8), 8)
        copy = pltpu.make_async_copy(view.at[:, part, :], next_hbm.at[:, part, :], left.at[group])
        copy.start()
        copies.append(copy)
    for copy in copies:
        copy.wait()


def finish(gram, split):
    return pl.pallas_call(
        finish_kernel,
        out_shape=(
            jax.ShapeDtypeStruct((3, PROBES, PROBES), F32),
            jax.ShapeDtypeStruct((3, PROBES, PROBES), F32),
            jax.ShapeDtypeStruct((PROBES, CELLS, LANES), F32),
        ),
        in_specs=vmem_specs(2),
        out_specs=(pl.BlockSpec(memory_space=pltpu.HBM),) * 3,
        scratch_shapes=[
            pltpu.VMEM((PROBES * CELLS, LANES), F32),
            pltpu.VMEM((3, PROBES, PROBES), F32),
            pltpu.VMEM((3, PROBES, PROBES), F32),
            pltpu.SemaphoreType.DMA((CELLS // 8,)),
            pltpu.SemaphoreType.DMA((2,)),
        ],
        compiler_params=pltpu.CompilerParams(vmem_limit_bytes=VMEM_LIMIT),
        interpret=INTERPRET,
        name="finish",
    )(*held(gram, split))


def off_chip(x):
    count = lax.axis_size(GX)
    return lax.ppermute(x, GX, [(i, (i - 1 if i % 2 == 0 else i + 1) % count) for i in range(count)])


def on_chip(x):
    count = lax.axis_size(CORE)
    return lax.ppermute(x, CORE, [(i, count - 1 - i) for i in range(count)])


def row_pair(x, offset):
    count = lax.axis_size(GY)
    step = lambda i: i + 1 if i % 2 == offset else i - 1
    return lax.ppermute(x, GY, [(i, step(i) % count) for i in range(count)])


def exchanged(x, axes):
    return lax.all_to_all(x, axes, 0, 0, tiled=True)


def gathered(x, axes):
    return exchanged(jnp.broadcast_to(x[None], (lax.axis_size(axes),) + x.shape), axes)


def reduced(x):
    near = lax.axis_size(NEAR)
    part = exchanged(x.reshape(near, x.shape[0] // near, x.shape[1]), NEAR).sum(0)
    part = gathered(part, FAR).sum(0)
    return gathered(part, NEAR).reshape(x.shape)


def per_device(probe_signs, diagonal):
    signs = probe_signs.reshape(PROBES * CELLS, LANES)
    diag = diagonal.reshape(CELLS, LANES)
    own, top, bottom = prepare(signs, diag)
    high = row_pair(top, 0)
    low = row_pair(bottom, 1)
    near = off_chip(own)
    beside = on_chip(own)
    corner_message = pack(0, ROWS, high, low, beside)
    corner = off_chip(corner_message)
    cross_message = pack(1, 0, high, low, near)
    cross = on_chip(cross_message)
    split, first, second = basis_early(own, high, low, near, beside)
    split, gram = basis_late(own, high, low, near, beside, corner, cross, first, second, split)
    alphas, betas, following = finish(reduced(gram), split)
    return (alphas, betas, following.reshape(PROBES, PLANES, ROWS, LANES))


def solution(mesh):
    split = Mesh(mesh.devices.reshape(2, 8, 2, 8, 2), ("gx_0", "gx_1", "gx_2", "gy_0", "gy_1"))
    placed = (P(None, GX, GY, None), P(GX, GY, None))
    return jax.shard_map(
        per_device,
        mesh=split,
        in_specs=placed,
        out_specs=(P(), P(), P(None, GX, GY, None)),
        check_vma=False,
    )
```

```python
import functools

import jax
import jax.numpy as jnp
from jax import lax
from jax.experimental import pallas as pl
from jax.experimental.pallas import tpu as pltpu
from jax.sharding import Mesh
from jax.sharding import PartitionSpec as P


GX = ("gx_0", "gx_1", "gx_2")
GY = ("gy_0", "gy_1")
NEAR = ("gx_0", "gx_2", "gy_1")
FAR = ("gx_1", "gy_0")
CORE = "gx_2"
PAIR = "gy_1"

PROBES = 32
LANES = 128
ROWS = 16
PLANES = 2
CELLS = PLANES * ROWS
SHIFT = 7.75
B0 = 7.0
B1 = 10.0
PANEL = 8
F32 = jnp.float32
BF16 = jnp.bfloat16
INTERPRET = False
VMEM_LIMIT = 16 * 2**20

OWN_ROWS = CELLS * PROBES + CELLS
EDGE_ROWS = 2 * 3 * PROBES + 8
MESSAGE_ROWS = (ROWS + 6) * PROBES + 8


def vmem_specs(count):
    return [pl.BlockSpec(memory_space=pltpu.VMEM) for _ in range(count)]


def shaped(*shape, dtype=F32):
    return pltpu.VMEM(shape, dtype)


def held(*arrays):
    return tuple(pltpu.with_memory_space_constraint(x, pltpu.VMEM) for x in arrays)


def row_of(index):
    return pl.ds(index * PROBES, PROBES)


def mirrored():
    core = lax.axis_index(CORE)
    pair = lax.axis_index(PAIR)

    def position(plane, row):
        return (plane + core * (1 - 2 * plane)) * ROWS + row + pair * (ROWS - 1 - 2 * row)

    return position


def prepare_kernel(
    signs_hbm, diag_hbm, own_ref, high_ref, low_ref, signs_ref, diag_ref, arrived
):
    rows = 8 * CELLS
    copies = []
    for group in range(PROBES // 8):
        part = pl.ds(group * rows, rows)
        copies.append(pltpu.make_async_copy(signs_hbm.at[part, :], signs_ref.at[part, :], arrived.at[group]))
    lines = pltpu.make_async_copy(diag_hbm, diag_ref, arrived.at[PROBES // 8])
    lines.start()
    for copy in copies:
        copy.start()
    position = mirrored()

    lines.wait()
    for cell in range(CELLS):
        plane, row = divmod(cell, ROWS)
        line = diag_ref[pl.ds(position(plane, row), 1), :]
        own_ref[CELLS * PROBES + cell : CELLS * PROBES + cell + 1, :] = line
        for ref, step in ((low_ref, row), (high_ref, ROWS - 1 - row)):
            if step < 2:
                start = 6 * PROBES + plane * 2 + step
                ref[start : start + 1, :] = line
    for ref in (low_ref, high_ref):
        ref[6 * PROBES + 4 :, :] = jnp.zeros((4, LANES), F32)
    for group in range(PROBES // 8):
        copies[group].wait()
        for cell in range(CELLS):
            plane, row = divmod(cell, ROWS)
            bits = signs_ref[pl.ds(group * rows + position(plane, row), 8, stride=CELLS), :]
            probes = (2 * bits - 1).astype(F32)

            def put(ref, index):
                ref[pl.ds(index * PROBES + group * 8, 8), :] = probes

            put(own_ref, cell)
            for ref, step in ((low_ref, row), (high_ref, ROWS - 1 - row)):
                if step < 3:
                    put(ref, plane * 3 + step)


def prepare(signs, diagonal):
    hbm = pl.BlockSpec(memory_space=pltpu.HBM)
    return pl.pallas_call(
        prepare_kernel,
        out_shape=(
            shaped(OWN_ROWS, LANES),
            shaped(EDGE_ROWS, LANES),
            shaped(EDGE_ROWS, LANES),
        ),
        in_specs=[hbm, hbm],
        out_specs=tuple(vmem_specs(3)),
        scratch_shapes=[
            pltpu.VMEM((PROBES * CELLS, LANES), jnp.int32),
            pltpu.VMEM((CELLS, LANES), F32),
            pltpu.SemaphoreType.DMA((PROBES // 8 + 1,)),
        ],
        compiler_params=pltpu.CompilerParams(vmem_limit_bytes=VMEM_LIMIT),
        interpret=INTERPRET,
        name="prepare",
    )(*(pltpu.with_memory_space_constraint(x, pltpu.HBM) for x in (signs, diagonal)))


def pack_kernel(plane, first_row, high_ref, low_ref, across_ref, message_ref):
    def edge(plane, row):
        if row < 0:
            return low_ref[row_of(plane * 3 - row - 1), :]
        return high_ref[row_of(plane * 3 + row - ROWS), :]

    for row in range(ROWS):
        message_ref[row_of(row), :] = across_ref[row_of(first_row + row), :]
    for place, row in enumerate((-2, -1, ROWS, ROWS + 1)):
        message_ref[row_of(ROWS + place), :] = edge(plane, row)
    for place, row in enumerate((-1, ROWS)):
        message_ref[row_of(ROWS + 4 + place), :] = edge(1 - plane, row)
        start = (ROWS + 6) * PROBES + place
        source = low_ref if row < 0 else high_ref
        line = 6 * PROBES + plane * 2
        message_ref[start : start + 1, :] = source[line : line + 1, :]
    message_ref[(ROWS + 6) * PROBES + 2 :, :] = jnp.zeros((6, LANES), F32)


def pack(plane, first_row, *operands):
    return pl.pallas_call(
        functools.partial(pack_kernel, plane, first_row),
        out_shape=shaped(MESSAGE_ROWS, LANES),
        in_specs=vmem_specs(len(operands)),
        out_specs=vmem_specs(1)[0],
        compiler_params=pltpu.CompilerParams(vmem_limit_bytes=VMEM_LIMIT),
        interpret=INTERPRET,
    )(*held(*operands))


def nt_dot(left, right):
    return lax.dot_general(left, right, (((1,), (1,)), ((), ())), preferred_element_type=F32)


def moved(value, blocks):
    return pltpu.roll(value, (blocks * PROBES) % LANES, 1)


def places():
    row = lax.broadcasted_iota(jnp.int32, (PROBES, LANES), 0)
    lane = lax.broadcasted_iota(jnp.int32, (PROBES, LANES), 1)
    return row, lane, lane % PROBES


def packed(first, last):
    row, lane, column = places()
    other = moved(last, -1)
    diagonals = jnp.sum(jnp.where(row == column, other, 0.0), axis=0, keepdims=True)
    slanted = pltpu.roll(jnp.broadcast_to(diagonals, (8, LANES)), 0, 1, stride=16, stride_axis=0)
    slanted = jnp.concatenate([slanted] * (PROBES // 8), 0)
    held_here = (row >= 17) & (row < 23) & (lane >= 96) & (lane < 112)
    return jnp.where(row <= column, first, jnp.where(held_here, slanted, other))


def unpacked(value):
    row, lane, column = places()
    turned = value.T
    turned = jnp.concatenate([turned[block * PROBES : (block + 1) * PROBES, :] for block in range(4)], 1)
    slanted = jnp.zeros((8, LANES), F32)
    for step in range(1, 7):
        mine = (row[:8] == step) & (lane[:8] // 16 == 6 - step)
        slanted = jnp.where(mine, pltpu.roll(value[16:24, :], LANES - 16 * step, 1), slanted)
    diagonals = jnp.sum(slanted, axis=0, keepdims=True)
    first = jnp.where(row <= column, value, turned)
    other = jnp.where(row == column, diagonals, jnp.where(row > column, value, turned))
    return first, moved(other, 1)


def distance(plane):
    return -plane if plane < 0 else max(plane - (PLANES - 1), 0)


def cells(width):
    found = []
    for plane in range(-width, PLANES + width):
        extra = width - distance(plane)
        for row in range(-extra, ROWS + extra):
            found.append((plane, row))
    return found


def known_early(order, plane, row):
    if order == 0:
        return distance(plane) == 0 or (distance(plane) < 3 and 0 <= row < ROWS)
    around = [(plane, row), (plane - 1, row), (plane + 1, row), (plane, row - 1), (plane, row + 1)]
    return all(known_early(order - 1, *cell) for cell in around)


def slots(order, width, early):
    chosen = [cell for cell in cells(width) if known_early(order, *cell) == early]
    return {cell: slot for slot, cell in enumerate(chosen)}


FIRST_EARLY, FIRST_LATE = slots(1, 2, True), slots(1, 2, False)
SECOND_EARLY, SECOND_LATE = slots(2, 1, True), slots(2, 1, False)


class Fields:
    def __init__(self, own, high, low, near, beside, corner, cross, first, second, split):
        self.own, self.high, self.low, self.near, self.beside = own, high, low, near, beside
        self.corner, self.cross = corner, cross
        self.first, self.second, self.split = first, second, split

    def k0(self, plane, row):
        away = distance(plane)
        if away == 0:
            if row < 0:
                return self.low[row_of(plane * 3 - row - 1), :]
            if row >= ROWS:
                return self.high[row_of(plane * 3 + row - ROWS), :]
            return self.own[row_of(plane * ROWS + row), :]
        if away == 3:
            return (self.corner if plane < 0 else self.cross)[row_of(row), :]
        if 0 <= row < ROWS:
            if plane < 0:
                return self.near[row_of((away - 1) * ROWS + row), :]
            return self.beside[row_of((2 - away) * ROWS + row), :]
        ref = self.corner if plane < 0 else self.cross
        known = (-2, -1, ROWS, ROWS + 1) if away == 1 else (-1, ROWS)
        return ref[row_of(ROWS + 4 * (away - 1) + known.index(row)), :]

    def factor(self, plane, row):
        away = distance(plane)
        if away == 0:
            if row < 0:
                ref, start = self.low, 6 * PROBES + plane * 2 - row - 1
            elif row >= ROWS:
                ref, start = self.high, 6 * PROBES + plane * 2 + row - ROWS
            else:
                ref, start = self.own, CELLS * PROBES + plane * ROWS + row
        elif 0 <= row < ROWS:
            if plane < 0:
                ref, start = self.near, CELLS * PROBES + (away - 1) * ROWS + row
            else:
                ref, start = self.beside, CELLS * PROBES + (2 - away) * ROWS + row
        else:
            ref = self.corner if plane < 0 else self.cross
            start = (ROWS + 6) * PROBES + (0 if row < 0 else 1)
        return ref[start : start + 1, :] + (6.0 - SHIFT)

    def k1(self, plane, row):
        early = (plane, row) in FIRST_EARLY
        slot = (FIRST_EARLY if early else FIRST_LATE)[(plane, row)]
        return self.first[0 if early else 1][row_of(slot), :]

    def k2(self, plane, row):
        early = (plane, row) in SECOND_EARLY
        slot = (SECOND_EARLY if early else SECOND_LATE)[(plane, row)]
        return self.second[0 if early else 1][row_of(slot), :]

    def apply(self, field, plane, row):
        center = field(plane, row)
        beside = field(plane - 1, row) + field(plane + 1, row)
        beside = beside + (field(plane, row - 1) + field(plane, row + 1))
        beside = beside + (pltpu.roll(center, 1, 1) + pltpu.roll(center, LANES - 1, 1))
        return self.factor(plane, row) * center - beside

    def keep(self, order, plane, row, value):
        if distance(plane) > 0 or not 0 <= row < ROWS:
            return
        columns = pl.ds((plane * ROWS + row) * LANES, LANES)
        upper = value.astype(BF16)
        self.split[row_of(order), columns] = upper
        if order == 0:
            self.split[row_of(4), columns] = jnp.zeros_like(upper)
        else:
            self.split[row_of(order + 4), columns] = (value - upper.astype(F32)).astype(BF16)

    def fill(self, early):
        side = 0 if early else 1
        for (plane, row), slot in (FIRST_EARLY if early else FIRST_LATE).items():
            value = self.apply(self.k0, plane, row)
            self.first[side][row_of(slot), :] = value
            self.keep(1, plane, row, value)
        for (plane, row), slot in (SECOND_EARLY if early else SECOND_LATE).items():
            value = self.apply(self.k1, plane, row) - B0 * self.k0(plane, row)
            self.second[side][row_of(slot), :] = value
            self.keep(2, plane, row, value)


def start_kernel(own_ref, split_ref):
    fields = Fields(own_ref, None, None, None, None, None, None, None, None, split_ref)
    for plane, row in cells(0):
        fields.keep(0, plane, row, fields.k0(plane, row))


def basis_start(own):
    return pl.pallas_call(
        start_kernel,
        out_shape=shaped(8 * PROBES, CELLS * LANES, dtype=BF16),
        in_specs=vmem_specs(1),
        out_specs=vmem_specs(1)[0],
        compiler_params=pltpu.CompilerParams(vmem_limit_bytes=VMEM_LIMIT),
        interpret=INTERPRET,
        name="basis_start",
    )(*held(own))


def early_kernel(own_ref, high_ref, low_ref, near_ref, beside_ref, split_in, split_ref, first_ref, second_ref):
    fields = Fields(
        own_ref, high_ref, low_ref, near_ref, beside_ref, None, None, (first_ref, None), (second_ref, None), split_ref
    )
    fields.fill(True)


def late_kernel(
    own_ref, high_ref, low_ref, near_ref, beside_ref, corner_ref, cross_ref, first_ref, second_ref, split_in,
    split_ref, gram_ref, first_late, second_late,
):
    fields = Fields(
        own_ref, high_ref, low_ref, near_ref, beside_ref, corner_ref, cross_ref,
        (first_ref, first_late), (second_ref, second_late), split_ref,
    )
    fields.fill(False)
    for plane, row in cells(0):
        fields.keep(3, plane, row, fields.apply(fields.k2, plane, row) - B1 * fields.k1(plane, row))
    split = split_ref[...]
    left = jnp.concatenate([split[:PROBES], split[3 * PROBES : 4 * PROBES], split[7 * PROBES :]], 0)
    product = nt_dot(left, split)
    product = product[:, :LANES] + product[:, LANES:]
    gram_ref[...] = packed(product[:PROBES], product[PROBES : 2 * PROBES] + product[2 * PROBES :])


def basis_early(*operands):
    return pl.pallas_call(
        early_kernel,
        out_shape=(
            shaped(8 * PROBES, CELLS * LANES, dtype=BF16),
            shaped(len(FIRST_EARLY) * PROBES, LANES),
            shaped(len(SECOND_EARLY) * PROBES, LANES),
        ),
        in_specs=vmem_specs(len(operands)),
        out_specs=tuple(vmem_specs(3)),
        input_output_aliases={len(operands) - 1: 0},
        compiler_params=pltpu.CompilerParams(vmem_limit_bytes=VMEM_LIMIT),
        interpret=INTERPRET,
        name="basis_early",
    )(*held(*operands))


def basis_late(*operands):
    return pl.pallas_call(
        late_kernel,
        out_shape=(shaped(8 * PROBES, CELLS * LANES, dtype=BF16), shaped(PROBES, LANES)),
        in_specs=vmem_specs(len(operands)),
        out_specs=tuple(vmem_specs(2)),
        scratch_shapes=[
            pltpu.VMEM((len(FIRST_LATE) * PROBES, LANES), F32),
            pltpu.VMEM((len(SECOND_LATE) * PROBES, LANES), F32),
        ],
        input_output_aliases={len(operands) - 1: 0},
        compiler_params=pltpu.CompilerParams(vmem_limit_bytes=VMEM_LIMIT),
        interpret=INTERPRET,
        name="basis_late",
    )(*held(*operands))


def eliminate(system, block):
    groups = PROBES // 8
    lane = lax.broadcasted_iota(jnp.int32, (8, LANES), 1)
    sub = lax.broadcasted_iota(jnp.int32, (8, LANES), 0)
    start = block * PROBES
    inside = (lane >= start) & (lane < start + PROBES)
    pivoted = [system[8 * g : 8 * g + 8, :] for g in range(groups)]
    solved = [
        jnp.where(inside, jnp.where(lane - start == sub + 8 * g, 1.0, 0.0), pivoted[g]) for g in range(groups)
    ]
    scales = [None] * PROBES
    spread = {}

    def spread_panel(panel):
        for k in range(panel, min(panel + PANEL, PROBES)):
            for g in range(max(panel - PANEL, 0) // 8, groups):
                column = pivoted[g][:, start + k : start + k + 1]
                spread[k, g] = jnp.broadcast_to(column, (8, LANES))

    spread_panel(0)
    for panel in range(0, PROBES, PANEL):
        spread_panel(panel + PANEL)
        for k in range(panel, panel + PANEL):
            group, line = divmod(k, 8)

            def pivot_row(value):
                return jnp.broadcast_to(value[line : line + 1, :], (8, LANES))

            pivot = pivot_row(spread[k, group])
            inverse = 1.0 / pivot
            scales[k] = lax.rsqrt(pivot)
            multiplier = {}
            for g in range(group, groups):
                value = spread[k, g] * inverse
                if g == group:
                    value = jnp.where(sub > line, value, 0.0)
                multiplier[g] = value
            row = pivot_row(pivoted[group])
            solved_row = pivot_row(solved[group])
            for other in range(k + 1, min(panel + 2 * PANEL, PROBES)):
                weight = pivot_row(spread[other, group])
                for g in range(group, groups):
                    spread[other, g] = spread[other, g] - multiplier[g] * weight
            for g in range(group, groups):
                pivoted[g] = pivoted[g] - multiplier[g] * row
                solved[g] = solved[g] - multiplier[g] * solved_row
    upper = []
    for g in range(groups):
        scale = scales[8 * g]
        for line in range(1, 8):
            scale = jnp.where(sub == line, scales[8 * g + line], scale)
        solved[g] = solved[g] * scale
        upper.append(jnp.where(inside & (lane - start >= sub + 8 * g), pivoted[g] * scale, 0.0))
    return jnp.concatenate(solved, 0), jnp.concatenate(upper, 0)


def parts_of(value):
    upper = value.astype(BF16)
    rest = value - upper.astype(F32)
    middle = rest.astype(BF16)
    return upper, middle, (rest - middle.astype(F32)).astype(BF16)


def square(value):
    upper, middle, lower = parts_of(value)
    left = jnp.concatenate([upper, upper, middle, middle, upper, lower], 0)
    right = jnp.concatenate([upper, middle, upper, middle, lower, upper], 0)
    return lax.dot_general(left, right, (((0,), (0,)), ((), ())), preferred_element_type=F32)


def wide_dot(left, right):
    left_upper, left_lower, _ = parts_of(left)
    right_upper, right_lower, _ = parts_of(right)
    both = jnp.concatenate([left_upper, left_lower], 1)
    result = nt_dot(both, jnp.concatenate([right_upper, right_upper], 1))
    return result + nt_dot(both, jnp.concatenate([right_lower, right_lower], 1))


def finish_kernel(
    gram_ref, split_ref, alpha_hbm, beta_hbm, next_hbm, next_ref, alpha_ref, beta_ref, left, sent
):
    lane = lax.broadcasted_iota(jnp.int32, (PROBES, LANES), 1)
    block_of = lane // PROBES
    first, last = unpacked(gram_ref[...])
    second = moved(first, -1) + jnp.where(block_of == 1, B0, B1) * moved(first, 1)
    second = jnp.where(block_of == 3, moved(last, 2), jnp.where(block_of == 0, 0.0, second))
    third = moved(last, 1) + jnp.where(block_of == 2, B1 * moved(second, 1) - B0 * first, 0.0)
    third = jnp.where(block_of < 2, 0.0, third)
    systems = [first, second, third, jnp.where(block_of < 3, 0.0, last)]
    row32 = lax.broadcasted_iota(jnp.int32, (PROBES, PROBES), 0)
    lane32 = lax.broadcasted_iota(jnp.int32, (PROBES, PROBES), 1)
    solved = []
    beta = None
    for block in range(4):
        value, triangle = eliminate(systems[block], block)
        solved.append(value)
        if block < 3:
            update = square(value)
            for later in range(block + 1, 4):
                change = update[later * PROBES : (later + 1) * PROBES, :]
                change = jnp.where((block_of <= block) | (block_of >= later), change, 0.0)
                systems[later] = systems[later] - change
        if block > 0:
            beta = wide_dot(moved(triangle, -1), inverse)
            beta_ref[block - 1] = jnp.where(row32 <= lane32, beta, 0.0)
        if block < 3:
            inverse = jnp.where(block_of == block, value, 0.0)
            alpha = wide_dot(moved(value, -1), inverse)
            if block > 0:
                coupled = wide_dot(solved[block - 1], inverse)
                alpha = alpha - jnp.dot(
                    beta, coupled, precision=lax.Precision.HIGHEST, preferred_element_type=F32
                )
            alpha_ref[block] = alpha + jnp.where(row32 == lane32, SHIFT, 0.0)
    upper, lower, _ = parts_of(solved[3])
    weights = jnp.concatenate(
        [jnp.concatenate([upper, upper], 1), jnp.concatenate([lower, jnp.zeros_like(lower)], 1)], 0
    )
    position = mirrored()
    view = next_ref.reshape(PROBES, CELLS, LANES)
    copies = [
        pltpu.make_async_copy(alpha_ref, alpha_hbm, sent.at[0]),
        pltpu.make_async_copy(beta_ref, beta_hbm, sent.at[1]),
    ]
    for copy in copies:
        copy.start()
    for group in range(CELLS // 8):
        columns = pl.ds(group * 8 * LANES, 8 * LANES)
        result = jnp.dot(weights, split_ref[:, columns], preferred_element_type=F32)
        result = result[:PROBES] + result[PROBES:]
        for place in range(8):
            plane, row = divmod(group * 8 + place, ROWS)
            target = pl.ds(position(plane, row), PROBES, stride=CELLS)
            next_ref[target, :] = result[:, place * LANES : (place + 1) * LANES]
        plane, half = divmod(group, 2)
        core, pair = lax.axis_index(CORE), lax.axis_index(PAIR)
        first = (plane + core * (1 - 2 * plane)) * ROWS + (half + pair * (1 - 2 * half)) * 8
        part = pl.ds(pl.multiple_of(first, 8), 8)
        copy = pltpu.make_async_copy(view.at[:, part, :], next_hbm.at[:, part, :], left.at[group])
        copy.start()
        copies.append(copy)
    for copy in copies:
        copy.wait()


def finish(gram, split):
    return pl.pallas_call(
        finish_kernel,
        out_shape=(
            jax.ShapeDtypeStruct((3, PROBES, PROBES), F32),
            jax.ShapeDtypeStruct((3, PROBES, PROBES), F32),
            jax.ShapeDtypeStruct((PROBES, CELLS, LANES), F32),
        ),
        in_specs=vmem_specs(2),
        out_specs=(pl.BlockSpec(memory_space=pltpu.HBM),) * 3,
        scratch_shapes=[
            pltpu.VMEM((PROBES * CELLS, LANES), F32),
            pltpu.VMEM((3, PROBES, PROBES), F32),
            pltpu.VMEM((3, PROBES, PROBES), F32),
            pltpu.SemaphoreType.DMA((CELLS // 8,)),
            pltpu.SemaphoreType.DMA((2,)),
        ],
        compiler_params=pltpu.CompilerParams(vmem_limit_bytes=VMEM_LIMIT),
        interpret=INTERPRET,
        name="finish",
    )(*held(gram, split))


def off_chip(x):
    count = lax.axis_size(GX)
    return lax.ppermute(x, GX, [(i, (i - 1 if i % 2 == 0 else i + 1) % count) for i in range(count)])


def on_chip(x):
    count = lax.axis_size(CORE)
    return lax.ppermute(x, CORE, [(i, count - 1 - i) for i in range(count)])


def row_pair(x, offset):
    count = lax.axis_size(GY)
    step = lambda i: i + 1 if i % 2 == offset else i - 1
    return lax.ppermute(x, GY, [(i, step(i) % count) for i in range(count)])


def exchanged(x, axes):
    return lax.all_to_all(x, axes, 0, 0, tiled=True)


def gathered(x, axes):
    return exchanged(jnp.broadcast_to(x[None], (lax.axis_size(axes),) + x.shape), axes)


def reduced(x):
    near = lax.axis_size(NEAR)
    part = exchanged(x.reshape(near, x.shape[0] // near, x.shape[1]), NEAR).sum(0)
    part = gathered(part, FAR).sum(0)
    return gathered(part, NEAR).reshape(x.shape)


def per_device(probe_signs, diagonal):
    signs = probe_signs.reshape(PROBES * CELLS, LANES)
    diag = diagonal.reshape(CELLS, LANES)
    own, top, bottom = prepare(signs, diag)
    high = row_pair(top, 0)
    low = row_pair(bottom, 1)
    near = off_chip(own)
    beside = on_chip(own)
    split = basis_start(own)
    corner_message = pack(0, ROWS, high, low, beside)
    corner = off_chip(corner_message)
    cross_message = pack(1, 0, high, low, near)
    cross = on_chip(cross_message)
    split, first, second = basis_early(own, high, low, near, beside, split)
    split, gram = basis_late(own, high, low, near, beside, corner, cross, first, second, split)
    alphas, betas, following = finish(reduced(gram), split)
    return (alphas, betas, following.reshape(PROBES, PLANES, ROWS, LANES))


def solution(mesh):
    split = Mesh(mesh.devices.reshape(2, 8, 2, 8, 2), ("gx_0", "gx_1", "gx_2", "gy_0", "gy_1"))
    placed = (P(None, GX, GY, None), P(GX, GY, None))
    return jax.shard_map(
        per_device,
        mesh=split,
        in_specs=placed,
        out_specs=(P(), P(), P(None, GX, GY, None)),
        check_vma=False,
    )
```
